8 devices in a mesh: dp: 2 (over z, y), tp: 4 (over x, core).
Axes of the slice: x: 2, y: 2, z: 1, core: 2. Of those that a mesh axis runs over, the one named last changes fastest.
Arguments:
- hidden: bfloat16 [2, 256, 3584], P('dp', 'tp'), parts along dimension 0
- positions: int32 [2, 256], P('dp'), parts along dimension 0
- gain_attn: bfloat16 [3584], replicated
- w_q: bfloat16 [3584, 3584], P(None, 'tp')
- b_q: bfloat16 [3584], P('tp')
- w_k: bfloat16 [3584, 512], P(None, 'tp')
- b_k: bfloat16 [512], P('tp')
- w_v: bfloat16 [3584, 512], P(None, 'tp')
- b_v: bfloat16 [512], P('tp')
- w_o: bfloat16 [3584, 3584], P('tp')
- gain_mlp: bfloat16 [3584], replicated
- w_gate: bfloat16 [3584, 18944], P(None, 'tp')
- w_up: bfloat16 [3584, 18944], P(None, 'tp')
- w_down: bfloat16 [18944, 3584], P('tp')
Outputs:
- output 1: bfloat16 [2, 256, 3584], P('dp', 'tp'), parts along dimension 0
- output 2: bfloat16 [2, 256, 4, 128], P('dp', None, 'tp'), parts along dimension 0
- output 3: bfloat16 [2, 256, 4, 128], P('dp', None, 'tp'), parts along dimension 0
There are 2 independent parts. The reference program is written for one: setup_inputs(seed, part) draws one part's arguments, and reference() takes and returns one part's arrays. A program takes and returns all parts, laid end to end along the dimension named above; an argument that names none is the same for every part.
All inputs are finite; a program needn't handle non-finite values.
Results may differ from the reference program's by a relative error of at most 0.0126876.
Values are sent between devices in bfloat16 or wider.
A program may use at most 1 GiB of HBM per device.

```python
import jax
import jax.numpy as jnp
from jax import lax

N_BATCH = 1
SEQ_LEN = 256
D_MODEL = 3584
N_HEADS = 28
N_KV_HEADS = 4
HEAD_DIM = 128
FF_DIM = 18944

GROUP_SIZE = N_HEADS // N_KV_HEADS
ROPE_THETA = 1000000.0
NORM_EPS = 1e-6


def normal_draw(rng_key, shape, scale):
    return (jax.random.normal(rng_key, shape, jnp.float32) * scale).astype(jnp.bfloat16)


def gain_draw(rng_key):
    return (0.5 + jax.random.uniform(rng_key, (D_MODEL,), jnp.float32)).astype(jnp.bfloat16)


def setup_inputs(seed: int = 0, part: int = 0) -> dict:
    base_key = jax.random.key(seed)
    part_key = jax.random.fold_in(base_key, part)
    hidden_key, start_key = jax.random.split(part_key, 2)
    key_list = jax.random.split(base_key, 12)
    q_width = N_HEADS * HEAD_DIM
    kv_width = N_KV_HEADS * HEAD_DIM
    start_pos = jax.random.randint(start_key, (N_BATCH, 1), 0, 2 * SEQ_LEN, dtype=jnp.int32)
    return {
        'hidden': normal_draw(hidden_key, (N_BATCH, SEQ_LEN, D_MODEL), 1.0),
        'positions': start_pos + jnp.arange(SEQ_LEN, dtype=jnp.int32)[None, :],
        'gain_attn': gain_draw(key_list[0]),
        'w_q': normal_draw(key_list[1], (D_MODEL, q_width), 1.5 * D_MODEL ** -0.5),
        'b_q': normal_draw(key_list[2], (q_width,), 0.3),
        'w_k': normal_draw(key_list[3], (D_MODEL, kv_width), 1.5 * D_MODEL ** -0.5),
        'b_k': normal_draw(key_list[4], (kv_width,), 0.3),
        'w_v': normal_draw(key_list[5], (D_MODEL, kv_width), D_MODEL ** -0.5),
        'b_v': normal_draw(key_list[6], (kv_width,), 0.3),
        'w_o': normal_draw(key_list[7], (q_width, D_MODEL), q_width ** -0.5),
        'gain_mlp': gain_draw(key_list[8]),
        'w_gate': normal_draw(key_list[9], (D_MODEL, FF_DIM), D_MODEL ** -0.5),
        'w_up': normal_draw(key_list[10], (D_MODEL, FF_DIM), D_MODEL ** -0.5),
        'w_down': normal_draw(key_list[11], (FF_DIM, D_MODEL), FF_DIM ** -0.5),
    }


def rms_norm(values, gain):
    values_f32 = values.astype(jnp.float32)
    inv_rms = lax.rsqrt(jnp.mean(values_f32 * values_f32, axis=-1, keepdims=True) + NORM_EPS)
    return (values_f32 * inv_rms * gain.astype(jnp.float32)).astype(jnp.bfloat16)


def rotary(values, positions):
    half_dim = HEAD_DIM // 2
    inv_freq = ROPE_THETA ** (-jnp.arange(half_dim, dtype=jnp.float32) / half_dim)
    angles = positions.astype(jnp.float32)[:, :, None] * inv_freq
    angles = angles.reshape(angles.shape[:2] + (1,) * (values.ndim - 3) + (half_dim,))
    cosine = jnp.cos(angles)
    sine = jnp.sin(angles)
    first = values[..., :half_dim]
    second = values[..., half_dim:]
    return jnp.concatenate([first * cosine - second * sine, second * cosine + first * sine], axis=-1)


def reference(hidden, positions, gain_attn, w_q, b_q, w_k, b_k, w_v, b_v, w_o, gain_mlp, w_gate, w_up, w_down):
    tokens = N_BATCH * SEQ_LEN
    normed = rms_norm(hidden, gain_attn).reshape(tokens, D_MODEL)
    query = jnp.dot(normed, w_q, preferred_element_type=jnp.float32) + b_q.astype(jnp.float32)
    key_proj = jnp.dot(normed, w_k, preferred_element_type=jnp.float32) + b_k.astype(jnp.float32)
    value_proj = jnp.dot(normed, w_v, preferred_element_type=jnp.float32) + b_v.astype(jnp.float32)
    query = rotary(query.reshape(N_BATCH, SEQ_LEN, N_HEADS, HEAD_DIM), positions).astype(jnp.bfloat16)
    k_cache = rotary(key_proj.reshape(N_BATCH, SEQ_LEN, N_KV_HEADS, HEAD_DIM), positions).astype(jnp.bfloat16)
    v_cache = value_proj.reshape(N_BATCH, SEQ_LEN, N_KV_HEADS, HEAD_DIM).astype(jnp.bfloat16)
    query_groups = query.reshape(N_BATCH, SEQ_LEN, N_KV_HEADS, GROUP_SIZE, HEAD_DIM).transpose(0, 2, 1, 3, 4).reshape(N_BATCH * N_KV_HEADS, SEQ_LEN, GROUP_SIZE, HEAD_DIM)
    key_groups = k_cache.transpose(0, 2, 1, 3).reshape(N_BATCH * N_KV_HEADS, SEQ_LEN, HEAD_DIM)
    value_groups = v_cache.transpose(0, 2, 1, 3).reshape(N_BATCH * N_KV_HEADS, SEQ_LEN, HEAD_DIM)
    causal = jnp.arange(SEQ_LEN)[:, None] >= jnp.arange(SEQ_LEN)[None, :]
    score_scale = HEAD_DIM ** -0.5

    def attend(operands):
        q_grp, k_grp, v_grp = operands
        scores = jnp.einsum('tgd,sd->gts', q_grp.astype(jnp.float32), k_grp.astype(jnp.float32)) * score_scale
        scores = jnp.where(causal[None], scores, -1e30)
        attn_probs = jax.nn.softmax(scores, axis=-1).astype(jnp.bfloat16).astype(jnp.float32)
        return jnp.einsum('gts,sd->tgd', attn_probs, v_grp.astype(jnp.float32)).astype(jnp.bfloat16)

    attn_out = lax.map(attend, (query_groups, key_groups, value_groups))
    attn_out = attn_out.reshape(N_BATCH, N_KV_HEADS, SEQ_LEN, GROUP_SIZE, HEAD_DIM).transpose(0, 2, 1, 3, 4).reshape(tokens, N_HEADS * HEAD_DIM)
    residual = hidden.reshape(tokens, D_MODEL).astype(jnp.float32)
    hidden_mid = (residual + jnp.dot(attn_out, w_o, preferred_element_type=jnp.float32)).astype(jnp.bfloat16)
    normed_mid = rms_norm(hidden_mid, gain_mlp)
    gate = jnp.dot(normed_mid, w_gate, preferred_element_type=jnp.float32)
    up_proj = jnp.dot(normed_mid, w_up, preferred_element_type=jnp.float32)
    activation = (jax.nn.silu(gate) * up_proj).astype(jnp.bfloat16)
    down_proj = jnp.dot(activation, w_down, preferred_element_type=jnp.float32)
    hidden_out = (hidden_mid.astype(jnp.float32) + down_proj).astype(jnp.bfloat16)
    return (hidden_out.reshape(N_BATCH, SEQ_LEN, D_MODEL), k_cache, v_cache)
```

```python
import jax
import jax.numpy as jnp
from jax import lax
from jax.experimental import pallas as pl
from jax.experimental.pallas import tpu as pltpu
from jax.sharding import PartitionSpec as P

HEAD_DIM = 128
ROPE_THETA = 1000000.0
NORM_EPS = 1e-6
D = 3584
HEADS = 7
QW = HEADS * HEAD_DIM
QKV = QW + 2 * HEAD_DIM
FF = 4736
NC = 7
CW = D // NC
BT = 64
T = 256
TW = 256
GS = 3
DS = 2
F32 = jnp.float32
BF16 = jnp.bfloat16
MESH = pl.DeviceIdType.MESH


def dot(a, b):
    return jnp.dot(a, b, preferred_element_type=F32)


def layer_kernel(x_h, pos_h, g1_h, wq_h, bq_h, wk_h, bk_h, wv_h, bv_h, wo_h, g2_h, wg_h, wu_h, wd_h, freq_h,
                 out_h, kc_h, vc_h,
                 xa, sta, gbuf, ubuf, pbuf, psib, sbuf, xs, obuf, hbuf, cprev, ssum, alpha, xs2, kvb,
                 g1, g2, bq, bk, bv, pos, freq,
                 sm_sem, x_sem, w_sem, wo_sem, g_sem, d_sem, o_sem,
                 xp_s, xp_r, xb_s, xb_r, xf_s, xf_r, st_s, st_r,
                 ps_s, ps_r, sx_s, sx_r, x1_s, x1_r, p2_s, p2_r, s2_s, s2_r):
    tp = lax.axis_index('tp')
    c = lax.div(tp, 2)
    k = lax.rem(tp, 2)
    oc = 1 - c
    ok = 1 - k
    sib = 2 * c + ok
    par = 2 * oc + k

    def remote(src, dst, ssem, rsem, target):
        return pltpu.make_async_remote_copy(src_ref=src, dst_ref=dst, send_sem=ssem, recv_sem=rsem,
                                            device_id={'tp': target}, device_id_type=MESH)

    def x_load(j):
        return pltpu.make_async_copy(x_h.at[0, :, pl.ds(j * CW, CW)], xa.at[j, c, k], x_sem.at[j])

    for j in range(NC):
        x_load(j).start()
    small = [(g1_h, g1), (g2_h, g2), (bq_h, bq), (bk_h, bk), (bv_h, bv), (pos_h, pos), (freq_h, freq)]
    small_cp = [pltpu.make_async_copy(s, d, sm_sem.at[i]) for i, (s, d) in enumerate(small)]
    for cp in small_cp:
        cp.start()

    def g_loads(j, slot):
        rows = pl.ds(pl.multiple_of(j * CW, CW), CW)
        return (pltpu.make_async_copy(wg_h.at[rows], gbuf.at[slot], g_sem.at[slot, 0]),
                pltpu.make_async_copy(wu_h.at[rows], ubuf.at[slot], g_sem.at[slot, 1]))

    def attention_half(wb, wob, qkv):
        def w_loads(j):
            rows = pl.ds(j * CW, CW)
            return (pltpu.make_async_copy(wq_h.at[rows], wb.at[j, :, pl.ds(0, QW)], w_sem.at[j, 0]),
                    pltpu.make_async_copy(wk_h.at[rows], wb.at[j, :, pl.ds(QW, HEAD_DIM)], w_sem.at[j, 1]),
                    pltpu.make_async_copy(wv_h.at[rows], wb.at[j, :, pl.ds(QW + HEAD_DIM, HEAD_DIM)], w_sem.at[j, 2]))

        for j in range(NC):
            for cp in w_loads(j):
                cp.start()
        wo_cp = pltpu.make_async_copy(wo_h, wob, wo_sem)
        wo_cp.start()
        for s in range(GS):
            for cp in g_loads(s, s):
                cp.start()

        barrier = pltpu.get_barrier_semaphore()
        for peer in (sib, par):
            pl.semaphore_signal(barrier, inc=1, device_id={'tp': peer}, device_id_type=MESH)
        pl.semaphore_wait(barrier, 2)

        def x_to_par(j):
            return remote(xa.at[j, c, k], xa.at[j, c, k], xp_s.at[j], xp_r.at[j], par)

        def x_from_par(j):
            return remote(xa.at[j, oc, k], xa.at[j, oc, k], xp_s.at[j], xp_r.at[j], par)

        def x_to_sib(j):
            return remote(xa.at[j, c, k], xa.at[j, c, k], xb_s.at[j], xb_r.at[j], sib)

        def x_from_sib(j):
            return remote(xa.at[j, c, ok], xa.at[j, c, ok], xb_s.at[j], xb_r.at[j], sib)

        def x_forward(j):
            return remote(xa.at[j, oc, k], xa.at[j, oc, k], xf_s.at[j], xf_r.at[j], sib)

        def x_forwarded(j):
            return remote(xa.at[j, oc, ok], xa.at[j, oc, ok], xf_s.at[j], xf_r.at[j], sib)

        x_load(0).wait()
        x_to_par(0).start()
        x_to_sib(0).start()
        square = jnp.zeros((BT, CW), F32)
        for j in range(NC):
            if j:
                x_load(j).wait()
            part = xa[j, c, k].astype(F32)
            square = square + part * part
        mean = jnp.sum(square, axis=-1, keepdims=True) / D
        inv = jnp.broadcast_to(lax.rsqrt(mean + NORM_EPS), (BT, 128))
        sta[c, k] = jnp.transpose(jnp.concatenate([inv, inv], axis=0))[:8]
        st_par = remote(sta.at[c, k], sta.at[c, k], st_s.at[0], st_r.at[0], par)
        st_par.start()
        st_sib = remote(sta.at[c, k], sta.at[c, k], st_s.at[1], st_r.at[1], sib)
        st_sib.start()
        for j in range(1, NC):
            x_to_par(j).start()
            x_to_sib(j).start()

        for cp in small_cp:
            cp.wait()
        pos_col = jnp.transpose(jnp.broadcast_to(pos[...].astype(F32), (HEAD_DIM, T)))
        angles = pos_col * freq[...]
        cosine = jnp.cos(angles)
        sine = jnp.sin(angles)
        lane = lax.broadcasted_iota(jnp.int32, (T, HEAD_DIM), 1)
        sine = jnp.where(lane < HEAD_DIM // 2, -sine, sine)

        remote(sta.at[oc, k], sta.at[oc, k], st_s.at[0], st_r.at[0], par).wait_recv()
        st_fwd = remote(sta.at[oc, k], sta.at[oc, k], st_s.at[2], st_r.at[2], sib)
        st_fwd.start()
        remote(sta.at[c, ok], sta.at[c, ok], st_s.at[1], st_r.at[1], sib).wait_recv()
        remote(sta.at[oc, ok], sta.at[oc, ok], st_s.at[2], st_r.at[2], sib).wait_recv()
        for cc in range(2):
            for kk in range(2):
                row = jnp.broadcast_to(sta[cc, kk][0:1], (128, 128))
                cprev[pl.ds((cc * 2 + kk) * BT, BT), :] = jnp.transpose(row)[:BT]
        qkv[...] = jnp.zeros_like(qkv)

        def project(j):
            x_from_sib(j).wait_recv()
            x_forwarded(j).wait_recv()
            for cp in w_loads(j):
                cp.wait()
            values = xa[j].reshape(T, CW).astype(F32)
            scale = jnp.concatenate([cprev[...]] * (CW // 128), axis=1)
            gain = g1[:, pl.ds(pl.multiple_of(j * CW, CW), CW)].astype(F32)
            hbuf[...] = (values * scale * gain).astype(BF16)
            qkv[...] += dot(hbuf[...], wb[j])

        x_from_par(0).wait_recv()
        x_forward(0).start()

        @pl.loop(1, NC)
        def _(j):
            x_from_par(j).wait_recv()
            x_forward(j).start()
            project(j - 1)

        project(NC - 1)

        def rotate(u):
            return u * cosine + pltpu.roll(u, HEAD_DIM // 2, 1) * sine

        key = rotate(qkv[:, pl.ds(QW, HEAD_DIM)] + bk[...].astype(F32)).astype(BF16)
        value = (qkv[:, pl.ds(QW + HEAD_DIM, HEAD_DIM)] + bv[...].astype(F32)).astype(BF16)
        kvb[0] = key
        kvb[1] = value
        k_out = pltpu.make_async_copy(kvb.at[0], kc_h, o_sem.at[NC])
        v_out = pltpu.make_async_copy(kvb.at[1], vc_h, o_sem.at[NC + 1])
        k_out.start()
        v_out.start()
        half = T // 2
        row_i = lax.broadcasted_iota(jnp.int32, (half, half), 0)
        col_i = lax.broadcasted_iota(jnp.int32, (half, half), 1)
        causal = row_i >= col_i
        for h in range(HEADS):
            cols = pl.ds(h * HEAD_DIM, HEAD_DIM)
            query = rotate(qkv[:, cols] + bq[:, cols].astype(F32)).astype(BF16)
            for r in range(2):
                width = half * (r + 1)
                scores = lax.dot_general(query[r * half:(r + 1) * half], key[:width], (((1,), (1,)), ((), ())),
                                         preferred_element_type=F32) * (HEAD_DIM ** -0.5)
                last = jnp.where(causal, scores[:, width - half:], -1e30)
                scores = last if r == 0 else jnp.concatenate([scores[:, :half], last], axis=1)
                weights = jnp.exp(scores - jnp.max(scores, axis=-1, keepdims=True))
                probs = (weights / jnp.sum(weights, axis=-1, keepdims=True)).astype(BF16)
                obuf[pl.ds(r * half, half), cols] = dot(probs, value[:width]).astype(BF16)

        wo_cp.wait()

        @pl.loop(0, NC)
        def _(j):
            cols = pl.ds(pl.multiple_of(j * CW, CW), CW)
            pbuf[j] = dot(obuf[...], wob[:, cols]).astype(BF16).reshape(2, 2, BT, CW)
            p_send(j).start()

        @pl.loop(0, NC)
        def _(j):
            x_to_par(j).wait_send()
            x_to_sib(j).wait_send()
            x_forward(j).wait_send()

        st_par.wait_send()
        st_sib.wait_send()
        st_fwd.wait_send()
        k_out.wait()
        v_out.wait()

    def p_send(j):
        return remote(pbuf.at[j, :, ok], psib.at[j], ps_s.at[j], ps_r.at[j], sib)

    pl.run_scoped(attention_half,
                  pltpu.VMEM((NC, CW, QKV), BF16), pltpu.VMEM((QW, D), BF16), pltpu.VMEM((T, QKV), F32))

    def mlp_half(accg, accu, act, dbuf):
        def d_load(j, slot):
            cols = pl.ds(pl.multiple_of(j * CW, CW), CW)
            return pltpu.make_async_copy(wd_h.at[:, cols], dbuf.at[slot], d_sem.at[slot])

        for s in range(DS):
            d_load(s, s).start()

        def s_send(j):
            return remote(sbuf.at[j], xs.at[j], sx_s.at[j], sx_r.at[j], par)

        def x1_send(j):
            return remote(xa.at[j, :, k], xa.at[j, :, k], x1_s.at[j], x1_r.at[j], sib)

        def x1_recv(j):
            return remote(xa.at[j, :, ok], xa.at[j, :, ok], x1_s.at[j], x1_r.at[j], sib)

        @pl.loop(0, NC)
        def _(j):
            p_send(j).wait_recv()
            sbuf[j] = (pbuf[j, :, k].astype(F32) + psib[j].astype(F32)).astype(BF16)
            s_send(j).start()

        def residual(j):
            s_send(j).wait_recv()
            total = sbuf[j].astype(F32) + xs[j].astype(F32)
            xa[j, :, k] = (xa[j, :, k].astype(F32) + total).astype(BF16)
            x1_send(j).start()

        def normalise(j, first):
            x1_recv(j).wait_recv()
            values = xa[j].reshape(T, CW).astype(F32)
            row_sum = jnp.sum(values * values, axis=-1, keepdims=True)
            if not first:
                row_sum = row_sum + ssum[...]
            ssum[...] = row_sum
            scale = lax.rsqrt(row_sum / ((j + 1) * CW) + NORM_EPS)
            wide = jnp.broadcast_to(scale, (T, 128))
            if not first:
                alpha[...] = wide / cprev[...]
            cprev[...] = wide
            gain = g2[:, pl.ds(pl.multiple_of(j * CW, CW), CW)].astype(F32)
            hbuf[...] = (values * scale * gain).astype(BF16)

        def put(mode, cols, dg, du):
            w = dg.shape[1]
            if mode != 'first':
                al = jnp.concatenate([alpha[...]] * (w // 128), axis=1)
                dg = accg[:, cols] * al + dg
                du = accu[:, cols] * al + du
            if mode == 'last':
                act[:, cols] = (dg / (1.0 + jnp.exp(-dg)) * du).astype(BF16)
            else:
                accg[:, cols] = dg
                accu[:, cols] = du

        def tiles(slot, mode, lo, hi):
            for n in range(lo, hi):
                cols = pl.ds(n * TW, TW)
                put(mode, cols, dot(hbuf[...], gbuf[slot, :, cols]), dot(hbuf[...], ubuf[slot, :, cols]))

        def tail(slot, mode):
            cols = pl.ds(FF - 128, 128)
            both = jnp.concatenate([gbuf[slot, :, cols], ubuf[slot, :, cols]], axis=1)
            res = dot(hbuf[...], both)
            put(mode, cols, res[:, :128], res[:, 128:])

        NT = FF // TW
        CUT = 11

        def gate_up(j, slot, mode):
            normalise(j, mode == 'first')
            for cp in g_loads(j, slot):
                cp.wait()
            tiles(slot, mode, 0, CUT)
            if mode != 'last':
                residual(j + 1)
            tiles(slot, mode, CUT, NT)
            tail(slot, mode)

        residual(0)
        gate_up(0, 0, 'first')
        for cp in g_loads(GS, 0):
            cp.start()

        @pl.loop(1, NC - 1)
        def _(j):
            slot = lax.rem(j, GS)
            gate_up(j, slot, 'mid')

            @pl.when(j + GS < NC)
            def _():
                for cp in g_loads(j + GS, slot):
                    cp.start()

        gate_up(NC - 1, (NC - 1) % GS, 'last')

        @pl.loop(0, NC)
        def _(j):
            p_send(j).wait_send()
            s_send(j).wait_send()

        def p2_send(j):
            return remote(pbuf.at[j, :, ok], psib.at[j], p2_s.at[j], p2_r.at[j], sib)

        def s2_send(j):
            return remote(sbuf.at[j, oc], xs2.at[j], s2_s.at[j], s2_r.at[j], par)

        def out_copy(j):
            cols = pl.ds(pl.multiple_of(j * CW, CW), CW)
            return pltpu.make_async_copy(sbuf.at[j, c], out_h.at[0, :, cols], o_sem.at[j])

        def down(j):
            slot = lax.rem(j, DS)
            d_load(j, slot).wait()
            pbuf[j] = dot(act[...], dbuf[slot]).astype(BF16).reshape(2, 2, BT, CW)
            p2_send(j).start()

        def chip_sum(j):
            p2_send(j).wait_recv()
            sbuf[j, oc] = (pbuf[j, oc, k].astype(F32) + psib[j, oc].astype(F32)).astype(BF16)
            s2_send(j).start()

        def finish(j):
            s2_send(j).wait_recv()
            total = pbuf[j, c, k].astype(F32) + psib[j, c].astype(F32) + xs2[j].astype(F32)
            sbuf[j, c] = (xa[j, c, k].astype(F32) + total).astype(BF16)
            out_copy(j).start()

        down(0)
        d_load(DS, 0).start()

        @pl.loop(1, NC)
        def _(j):
            down(j)

            @pl.when(j + DS < NC)
            def _():
                d_load(j + DS, lax.rem(j, DS)).start()

            chip_sum(j - 1)

        chip_sum(NC - 1)

        @pl.loop(0, NC)
        def _(j):
            finish(j)

        @pl.loop(0, NC)
        def _(j):
            x1_send(j).wait_send()
            p2_send(j).wait_send()
            s2_send(j).wait_send()
            out_copy(j).wait()

    pl.run_scoped(mlp_half,
                  pltpu.VMEM((T, FF), F32), pltpu.VMEM((T, FF), F32), pltpu.VMEM((T, FF), BF16),
                  pltpu.VMEM((DS, FF, CW), BF16))


def solution(mesh):
    def local_layer(hidden, positions, gain_attn, w_q, b_q, w_k, b_k, w_v, b_v, w_o, gain_mlp, w_gate, w_up, w_down):
        half = HEAD_DIM // 2
        freq = ROPE_THETA ** (-jnp.arange(half, dtype=F32) / half)
        freq = jnp.concatenate([freq, freq]).reshape(1, HEAD_DIM)
        dma = pltpu.SemaphoreType.DMA
        sems = [dma((7,)), dma((NC,)), dma((NC, 3)), dma, dma((GS, 2)), dma((DS,)), dma((NC + 2,)),
                dma((NC,)), dma((NC,)), dma((NC,)), dma((NC,)), dma((NC,)), dma((NC,)), dma((3,)), dma((3,))]
        sems += [dma((NC,)) for _ in range(10)]
        vm = pltpu.VMEM
        out, kc, vc = pl.pallas_call(
            layer_kernel,
            out_shape=(jax.ShapeDtypeStruct((1, BT, D), BF16), jax.ShapeDtypeStruct((T, HEAD_DIM), BF16),
                       jax.ShapeDtypeStruct((T, HEAD_DIM), BF16)),
            in_specs=[pl.BlockSpec(memory_space=pl.ANY)] * 15,
            out_specs=(pl.BlockSpec(memory_space=pl.ANY),) * 3,
            scratch_shapes=[
                vm((NC, 2, 2, BT, CW), BF16), vm((2, 2, 8, 128), F32),
                vm((GS, CW, FF), BF16), vm((GS, CW, FF), BF16),
                vm((NC, 2, 2, BT, CW), BF16), vm((NC, 2, BT, CW), BF16), vm((NC, 2, BT, CW), BF16), vm((NC, 2, BT, CW), BF16),
                vm((T, QW), BF16), vm((T, CW), BF16), vm((T, 128), F32), vm((T, 1), F32),
                vm((T, 128), F32), vm((NC, BT, CW), BF16), vm((2, T, HEAD_DIM), BF16),
                vm((1, D), BF16), vm((1, D), BF16), vm((1, QW), BF16), vm((1, HEAD_DIM), BF16), vm((1, HEAD_DIM), BF16),
                vm((1, T), jnp.int32), vm((1, HEAD_DIM), F32),
            ] + sems,
            compiler_params=pltpu.CompilerParams(collective_id=0, has_side_effects=True, vmem_limit_bytes=67043328),
            name='layer',
        )(hidden, positions, gain_attn.reshape(1, D), w_q, b_q.reshape(1, QW), w_k, b_k.reshape(1, HEAD_DIM), w_v,
          b_v.reshape(1, HEAD_DIM), w_o, gain_mlp.reshape(1, D), w_gate, w_up, w_down, freq)
        return out, kc.reshape(1, T, 1, HEAD_DIM), vc.reshape(1, T, 1, HEAD_DIM)

    token_rows = P('dp', 'tp', None)
    col_split = P(None, 'tp')
    row_split = P('tp', None)
    vec_split = P('tp')
    replicated = P(None)
    cache_spec = P('dp', None, 'tp', None)
    in_specs = (token_rows, P('dp', None), replicated, col_split, vec_split, col_split, vec_split, col_split, vec_split, row_split, replicated, col_split, col_split, row_split)
    out_specs = (token_rows, cache_spec, cache_spec)
    return jax.shard_map(local_layer, mesh=mesh, in_specs=in_specs, out_specs=out_specs, check_vma=False)
```

```python
import jax
import jax.numpy as jnp
import numpy as np
from jax import lax
from jax.experimental import pallas as pl
from jax.experimental.pallas import tpu as pltpu
from jax.sharding import PartitionSpec as P

HEAD_DIM = 128
ROPE_THETA = 1000000.0
NORM_EPS = 1e-6
D = 3584
HEADS = 7
QW = HEADS * HEAD_DIM
QKV = QW + 2 * HEAD_DIM
FF = 4736
NC = 7
CW = D // NC
BT = 64
T = 256
TW = 256
GH = 5
DS = 3
HW = CW // 2
UNITS = tuple((j, 0, CW) for j in range(NC))
NU = len(UNITS)
OUTS = tuple((j, 0, CW) for j in range(NC - 1)) + ((NC - 1, 0, HW), (NC - 1, HW, HW))
NO = len(OUTS)
F32 = jnp.float32
BF16 = jnp.bfloat16
MESH = pl.DeviceIdType.MESH


def add(parts):
    first, second = parts
    return first + second


def dot(a, b):
    return jnp.dot(a, b, preferred_element_type=F32)


def row(ref, start, size):
    if not isinstance(start, int):
        start = pl.multiple_of(start, size)
    return ref[pl.ds(start, size)].astype(F32).reshape(1, size)


def result_kernel(out_i, kc_i, vc_i, out_o, kc_o, vc_o, outb, kvb, i_sem, o_sem):
    loads = [(out_i.at[0, :, pl.ds(j * CW, CW)], outb.at[j]) for j in range(NC)] + [(kc_i, kvb.at[0]), (vc_i, kvb.at[1])]
    stores = [(outb.at[j], out_o.at[0, :, pl.ds(j * CW, CW)]) for j in range(NC)] + [(kvb.at[0], kc_o), (kvb.at[1], vc_o)]
    loads = [pltpu.make_async_copy(s, d, i_sem.at[i]) for i, (s, d) in enumerate(loads)]
    stores = [pltpu.make_async_copy(s, d, o_sem.at[i]) for i, (s, d) in enumerate(stores)]
    for cp in loads:
        cp.start()
    for load, store in zip(loads, stores):
        load.wait()
        store.start()
    for store in stores:
        store.wait()


def layer_kernel(x_h, pos_h, g1_h, wq_h, bq_h, wk_h, bk_h, wv_h, bv_h, wo_h, g2_h, wg_h, wu_h, wd_h, freq_h,
                 out_h, kc_h, vc_h,
                 xa, sta, gbuf, ubuf, pbuf, psib, sbuf, xs, obuf, hbuf, cprev, ssum, alpha, xs2,
                 g1, g2, bq, bk, bv, pos, freq,
                 sm_sem, x_sem, w_sem, wo_sem, g_sem, d_sem, o_sem,
                 xp_s, xp_r, xb_s, xb_r, xf_s, xf_r, st_s, st_r,
                 ps_s, ps_r, sx_s, sx_r, x1_s, x1_r, p2_s, p2_r, s2_s, s2_r):
    tp = lax.axis_index('tp')
    c = lax.div(tp, 2)
    k = lax.rem(tp, 2)
    oc = 1 - c
    ok = 1 - k
    sib = 2 * c + ok
    par = 2 * oc + k

    def remote(src, dst, ssem, rsem, target):
        return pltpu.make_async_remote_copy(src_ref=src, dst_ref=dst, send_sem=ssem, recv_sem=rsem,
                                            device_id={'tp': target}, device_id_type=MESH)

    def x_load(j):
        return pltpu.make_async_copy(x_h.at[0, :, pl.ds(j * CW, CW)], xa.at[j, c, k], x_sem.at[j])

    for j in range(NC):
        x_load(j).start()
    small = [(g1_h, g1), (g2_h, g2), (bq_h, bq), (bk_h, bk), (bv_h, bv), (pos_h, pos), (freq_h, freq)]
    small_cp = [pltpu.make_async_copy(s, d, sm_sem.at[i]) for i, (s, d) in enumerate(small)]
    for cp in small_cp:
        cp.start()

    def g_loads(i):
        slot = lax.rem(i, GH)
        rows = pl.ds(pl.multiple_of(i * HW, HW), HW)
        return (pltpu.make_async_copy(wg_h.at[rows], gbuf.at[slot], g_sem.at[slot, 0]),
                pltpu.make_async_copy(wu_h.at[rows], ubuf.at[slot], g_sem.at[slot, 1]))

    def attention_half(wb, wob, qkv):
        def w_loads(j):
            rows = pl.ds(j * CW, CW)
            return (pltpu.make_async_copy(wq_h.at[rows], wb.at[j, :, pl.ds(0, QW)], w_sem.at[j, 0]),
                    pltpu.make_async_copy(wk_h.at[rows], wb.at[j, :, pl.ds(QW, HEAD_DIM)], w_sem.at[j, 1]),
                    pltpu.make_async_copy(wv_h.at[rows], wb.at[j, :, pl.ds(QW + HEAD_DIM, HEAD_DIM)], w_sem.at[j, 2]))

        for j in range(NC):
            for cp in w_loads(j):
                cp.start()
        wo_cp = pltpu.make_async_copy(wo_h, wob, wo_sem)
        wo_cp.start()
        for i in range(GH):
            for cp in g_loads(i):
                cp.start()

        barrier = pltpu.get_barrier_semaphore()
        for peer in (sib, par):
            pl.semaphore_signal(barrier, inc=1, device_id={'tp': peer}, device_id_type=MESH)
        pl.semaphore_wait(barrier, 2)

        def x_to_par(j):
            return remote(xa.at[j, c, k], xa.at[j, c, k], xp_s.at[j], xp_r.at[j], par)

        def x_from_par(j):
            return remote(xa.at[j, oc, k], xa.at[j, oc, k], xp_s.at[j], xp_r.at[j], par)

        def x_to_sib(j):
            return remote(xa.at[j, c, k], xa.at[j, c, k], xb_s.at[j], xb_r.at[j], sib)

        def x_from_sib(j):
            return remote(xa.at[j, c, ok], xa.at[j, c, ok], xb_s.at[j], xb_r.at[j], sib)

        def x_forward(j):
            return remote(xa.at[j, oc, k], xa.at[j, oc, k], xf_s.at[j], xf_r.at[j], sib)

        def x_forwarded(j):
            return remote(xa.at[j, oc, ok], xa.at[j, oc, ok], xf_s.at[j], xf_r.at[j], sib)

        x_load(0).wait()
        x_to_par(0).start()
        x_to_sib(0).start()
        square = jnp.zeros((BT, CW), F32)
        for j in range(NC):
            if j:
                x_load(j).wait()
            part = xa[j, c, k].astype(F32)
            square = square + part * part
        mean = jnp.sum(square, axis=-1, keepdims=True) / D
        inv = jnp.broadcast_to(lax.rsqrt(mean + NORM_EPS), (BT, 128))
        sta[c, k] = jnp.transpose(jnp.concatenate([inv, inv], axis=0))[:8]
        st_par = remote(sta.at[c, k], sta.at[c, k], st_s.at[0], st_r.at[0], par)
        st_par.start()
        st_sib = remote(sta.at[c, k], sta.at[c, k], st_s.at[1], st_r.at[1], sib)
        st_sib.start()
        for j in range(1, NC):
            x_to_par(j).start()
            x_to_sib(j).start()

        for cp in small_cp:
            cp.wait()
        pos_col = jnp.transpose(jnp.broadcast_to(pos[...].astype(F32), (HEAD_DIM, T)))
        angles = pos_col * freq[...]
        cosine = jnp.cos(angles)
        sine = jnp.sin(angles)
        lane = lax.broadcasted_iota(jnp.int32, (T, HEAD_DIM), 1)
        sine = jnp.where(lane < HEAD_DIM // 2, -sine, sine)

        remote(sta.at[oc, k], sta.at[oc, k], st_s.at[0], st_r.at[0], par).wait_recv()
        st_fwd = remote(sta.at[oc, k], sta.at[oc, k], st_s.at[2], st_r.at[2], sib)
        st_fwd.start()
        remote(sta.at[c, ok], sta.at[c, ok], st_s.at[1], st_r.at[1], sib).wait_recv()
        remote(sta.at[oc, ok], sta.at[oc, ok], st_s.at[2], st_r.at[2], sib).wait_recv()
        for cc in range(2):
            for kk in range(2):
                wide = jnp.broadcast_to(sta[cc, kk][0:1], (128, 128))
                cprev[pl.ds((cc * 2 + kk) * BT, BT), :] = jnp.transpose(wide)[:BT]
        qkv[...] = jnp.zeros_like(qkv)

        def project(j):
            x_from_sib(j).wait_recv()
            x_forwarded(j).wait_recv()
            for cp in w_loads(j):
                cp.wait()
            values = xa[j].reshape(T, CW).astype(F32)
            scale = jnp.concatenate([cprev[...]] * (CW // 128), axis=1)
            gain = row(g1, j * CW, CW)
            hbuf[...] = (values * scale * gain).astype(BF16)
            qkv[...] += dot(hbuf[...], wb[j])

        x_from_par(0).wait_recv()
        x_forward(0).start()

        @pl.loop(1, NC)
        def _(j):
            x_from_par(j).wait_recv()
            x_forward(j).start()
            project(j - 1)

        project(NC - 1)

        def rotate(u):
            return u * cosine + pltpu.roll(u, HEAD_DIM // 2, 1) * sine

        key = rotate(qkv[:, pl.ds(QW, HEAD_DIM)] + row(bk, 0, HEAD_DIM)).astype(BF16)
        value = (qkv[:, pl.ds(QW + HEAD_DIM, HEAD_DIM)] + row(bv, 0, HEAD_DIM)).astype(BF16)
        key_lanes, value_lanes = pl.ds(0, HEAD_DIM), pl.ds(HEAD_DIM, HEAD_DIM)
        hbuf[:, key_lanes] = key
        hbuf[:, value_lanes] = value
        k_out = pltpu.make_async_copy(hbuf.at[:, key_lanes], kc_h, o_sem.at[NO])
        v_out = pltpu.make_async_copy(hbuf.at[:, value_lanes], vc_h, o_sem.at[NO + 1])
        k_out.start()
        v_out.start()
        half = T // 2
        rows = HEADS * half
        row_i = lax.rem(lax.broadcasted_iota(jnp.int32, (rows, half), 0), half)
        causal = row_i >= lax.broadcasted_iota(jnp.int32, (rows, half), 1)
        query = [rotate(qkv[:, pl.ds(h * HEAD_DIM, HEAD_DIM)] + row(bq, h * HEAD_DIM, HEAD_DIM)).astype(BF16)
                 for h in range(HEADS)]
        for r in range(2):
            width = half * (r + 1)
            stacked = jnp.concatenate([q[r * half:(r + 1) * half] for q in query], axis=0)
            scores = lax.dot_general(stacked, key[:width], (((1,), (1,)), ((), ())),
                                     preferred_element_type=F32) * (HEAD_DIM ** -0.5)
            last = jnp.where(causal, scores[:, width - half:], -1e30)
            scores = last if r == 0 else jnp.concatenate([scores[:, :half], last], axis=1)
            weights = jnp.exp(scores - jnp.max(scores, axis=-1, keepdims=True))
            probs = (weights * (1.0 / jnp.sum(weights, axis=-1, keepdims=True))).astype(BF16)
            out = dot(probs, value[:width]).astype(BF16)
            for h in range(HEADS):
                obuf[pl.ds(r * half, half), pl.ds(h * HEAD_DIM, HEAD_DIM)] = out[h * half:(h + 1) * half]

        wo_cp.wait()

        lag = 3
        for u, (j, lo, w) in enumerate(UNITS):
            part = dot(obuf[...], wob[:, pl.ds(j * CW + lo, w)]).astype(BF16)
            pbuf[j, :, :, :, pl.ds(lo, w)] = part.reshape(2, 2, BT, w)
            p_send(u, j, lo, w).start()
            if u >= lag:
                chip_partial(u - lag)
        for u in range(NU - lag, NU):
            chip_partial(u)

        @pl.loop(0, NC)
        def _(j):
            x_to_par(j).wait_send()
            x_to_sib(j).wait_send()
            x_forward(j).wait_send()

        st_par.wait_send()
        st_sib.wait_send()
        st_fwd.wait_send()
        k_out.wait()
        v_out.wait()

    def p_send(u, j, lo, w):
        lanes = pl.ds(lo, w)
        return remote(pbuf.at[j, :, ok, :, lanes], psib.at[j, :, :, lanes], ps_s.at[u], ps_r.at[u], sib)

    def s_send(u, j, lo, w):
        lanes = pl.ds(lo, w)
        return remote(sbuf.at[j, :, :, lanes], xs.at[j, :, :, lanes], sx_s.at[u], sx_r.at[u], par)

    def chip_partial(u):
        j, lo, w = UNITS[u]
        lanes = pl.ds(lo, w)
        p_send(u, j, lo, w).wait_recv()
        sbuf[j, :, :, lanes] = (pbuf[j, :, k, :, lanes].astype(F32) + psib[j, :, :, lanes].astype(F32)).astype(BF16)
        s_send(u, j, lo, w).start()

    pl.run_scoped(attention_half,
                  pltpu.VMEM((NC, CW, QKV), BF16), pltpu.VMEM((QW, D), BF16), pltpu.VMEM((T, QKV), F32))

    def mlp_half(accg, accu, act, dbuf):
        def d_load(j, slot):
            cols = pl.ds(pl.multiple_of(j * CW, CW), CW)
            return pltpu.make_async_copy(wd_h.at[:, cols], dbuf.at[slot], d_sem.at[slot])

        for s in range(DS):
            d_load(s, s).start()

        def x1_send(u, j, lo, w):
            part = xa.at[j, :, k, :, pl.ds(lo, w)]
            return remote(part, part, x1_s.at[u], x1_r.at[u], sib)

        def x1_recv(u, j, lo, w):
            part = xa.at[j, :, ok, :, pl.ds(lo, w)]
            return remote(part, part, x1_s.at[u], x1_r.at[u], sib)

        def residual(u, j, lo, w):
            lanes = pl.ds(lo, w)
            s_send(u, j, lo, w).wait_recv()
            total = sbuf[j, :, :, lanes].astype(F32) + xs[j, :, :, lanes].astype(F32)
            xa[j, :, k, :, lanes] = (xa[j, :, k, :, lanes].astype(F32) + total).astype(BF16)
            x1_send(u, j, lo, w).start()

        def normalise(u):
            values = xa[u].reshape(T, CW).astype(F32)
            row_sum = jnp.sum(values * values, axis=-1, keepdims=True)
            first = isinstance(u, int) and u == 0
            if not first:
                row_sum = row_sum + ssum[...]
            ssum[...] = row_sum
            scale = lax.rsqrt(row_sum / ((u + 1) * CW) + NORM_EPS)
            wide = jnp.broadcast_to(scale, (T, 128))
            if not first:
                alpha[...] = wide / cprev[...]
            cprev[...] = wide
            hbuf[...] = (values * scale * row(g2, u * CW, CW)).astype(BF16)

        def put(mode, rows, cols, dg, du):
            w = dg.shape[1]
            if mode != 'first':
                al = jnp.concatenate([alpha[rows, :]] * (w // 128), axis=1)
                dg = accg[rows, cols] * al + dg
                du = accu[rows, cols] * al + du
            if mode == 'last':
                act[rows, cols] = (dg / (1.0 + jnp.exp(-dg)) * du).astype(BF16)
            else:
                accg[rows, cols] = dg
                accu[rows, cols] = du

        def tiles(halves, mode, lo, hi):
            for n in range(lo, hi):
                cols = pl.ds(n * TW, TW)
                dg, du = [add([dot(hbuf[:, pl.ds(i * HW, HW)], ref[slot, :, cols]) for i, slot in enumerate(halves)])
                          for ref in (gbuf, ubuf)]
                put(mode, pl.ds(0, T), cols, dg, du)

        def tail(halves, mode):
            cols = pl.ds(FF - 128, 128)
            weight = [jnp.concatenate([gbuf[slot, :, cols], ubuf[slot, :, cols]], axis=1) for slot in halves]
            for r in range(2):
                rows = pl.ds(r * 2 * BT, 2 * BT)
                res = add([dot(hbuf[rows, pl.ds(i * HW, HW)], w) for i, w in enumerate(weight)])
                put(mode, rows, cols, res[:, :128], res[:, 128:])

        NT = FF // TW

        def gate_up(u, mode, cut):
            x1_recv(u, u, 0, CW).wait_recv()
            for i in range(2):
                for cp in g_loads(2 * u + i):
                    cp.wait()
            halves = [lax.rem(2 * u + i, GH) for i in range(2)]
            normalise(u)
            if mode == 'last':
                tiles(halves, mode, 0, NT)
            else:
                tiles(halves, mode, 0, cut)
                residual(u + 1, u + 1, 0, CW)
                tiles(halves, mode, cut, NT)
            tail(halves, mode)

        def refill(i):
            for cp in g_loads(i):
                cp.start()

        unit = [(u,) + UNITS[u] for u in range(NU)]
        residual(*unit[0])
        gate_up(0, 'first', 13)
        for i in range(2):
            refill(GH + i)

        @pl.loop(1, NC - 1)
        def _(u):
            gate_up(u, 'mid', 9)
            for i in range(2):
                @pl.when(2 * u + i + GH < 2 * NC)
                def _():
                    refill(2 * u + i + GH)

        gate_up(NC - 1, 'last', NT)

        for u in range(NU):
            p_send(*unit[u]).wait_send()
            s_send(*unit[u]).wait_send()

        def p2_send(u, j, lo, w):
            lanes = pl.ds(lo, w)
            return remote(pbuf.at[j, :, ok, :, lanes], psib.at[j, :, :, lanes], p2_s.at[u], p2_r.at[u], sib)

        def s2_send(u, j, lo, w):
            lanes = pl.ds(lo, w)
            return remote(sbuf.at[j, oc, :, lanes], xs2.at[j, :, lanes], s2_s.at[u], s2_r.at[u], par)

        def out_copy(u, j, lo, w):
            start = j * CW + lo
            cols = pl.ds(start if isinstance(start, int) else pl.multiple_of(start, CW), w)
            return pltpu.make_async_copy(sbuf.at[j, c, :, pl.ds(lo, w)], out_h.at[0, :, cols], o_sem.at[u])

        def down(u, j, lo, w):
            slot = lax.rem(j, DS)
            lanes = pl.ds(lo, w)
            if lo == 0:
                d_load(j, slot).wait()
            if w == CW:
                pbuf[j] = dot(act[...], dbuf[slot]).astype(BF16).reshape(2, 2, BT, w)
            else:
                for r in range(2):
                    part = dot(act[pl.ds(r * 2 * BT, 2 * BT), :], dbuf[slot, :, lanes])
                    pbuf[j, r, :, :, lanes] = part.astype(BF16).reshape(2, BT, w)
            p2_send(u, j, lo, w).start()

        def chip_sum(u, j, lo, w):
            lanes = pl.ds(lo, w)
            p2_send(u, j, lo, w).wait_recv()
            sbuf[j, oc, :, lanes] = (pbuf[j, oc, k, :, lanes].astype(F32) + psib[j, oc, :, lanes].astype(F32)).astype(BF16)
            s2_send(u, j, lo, w).start()

        def finish(u, j, lo, w):
            lanes = pl.ds(lo, w)
            s2_send(u, j, lo, w).wait_recv()
            total = pbuf[j, c, k, :, lanes].astype(F32) + psib[j, c, :, lanes].astype(F32) + xs2[j, :, lanes].astype(F32)
            sbuf[j, c, :, lanes] = (xa[j, c, k, :, lanes].astype(F32) + total).astype(BF16)
            out_copy(u, j, lo, w).start()

        outs = [(u,) + OUTS[u] for u in range(NO)]

        @pl.loop(0, NC - 1)
        def _(j):
            down(j, j, 0, CW)

            @pl.when(j + DS < NC)
            def _():
                d_load(j + DS, lax.rem(j, DS)).start()

            @pl.when(j > 0)
            def _():
                chip_sum(j - 1, j - 1, 0, CW)

        down(*outs[NO - 2])
        chip_sum(*outs[NO - 3])
        down(*outs[NO - 1])
        chip_sum(*outs[NO - 2])
        for u in range(NO - 4):
            finish(*outs[u])
        chip_sum(*outs[NO - 1])
        for u in range(NO - 4, NO):
            finish(*outs[u])

        for u in range(NU):
            x1_send(*unit[u]).wait_send()
        for u in range(NO):
            p2_send(*outs[u]).wait_send()
            s2_send(*outs[u]).wait_send()
            out_copy(*outs[u]).wait()

    pl.run_scoped(mlp_half,
                  pltpu.VMEM((T, FF), F32), pltpu.VMEM((T, FF), F32), pltpu.VMEM((T, FF), BF16),
                  pltpu.VMEM((DS, FF, CW), BF16))


def solution(mesh):
    def local_layer(hidden, positions, gain_attn, w_q, b_q, w_k, b_k, w_v, b_v, w_o, gain_mlp, w_gate, w_up, w_down):
        half = HEAD_DIM // 2
        freq = ROPE_THETA ** (-np.arange(half) / half)
        freq = np.concatenate([freq, freq]).reshape(1, HEAD_DIM).astype(np.float32)
        dma = pltpu.SemaphoreType.DMA
        sems = [dma((7,)), dma((NC,)), dma((NC, 3)), dma, dma((GH, 2)), dma((DS,)), dma((NO + 2,)),
                dma((NC,)), dma((NC,)), dma((NC,)), dma((NC,)), dma((NC,)), dma((NC,)), dma((3,)), dma((3,))]
        sems += [dma((NU,)) for _ in range(6)] + [dma((NO,)) for _ in range(4)]
        vm = pltpu.VMEM
        out, kc, vc = pl.pallas_call(
            layer_kernel,
            out_shape=(jax.ShapeDtypeStruct((1, BT, D), BF16), jax.ShapeDtypeStruct((T, HEAD_DIM), BF16),
                       jax.ShapeDtypeStruct((T, HEAD_DIM), BF16)),
            in_specs=[pl.BlockSpec(memory_space=pl.ANY)] * 15,
            out_specs=(pl.BlockSpec(memory_space=pl.ANY),) * 3,
            scratch_shapes=[
                vm((NC, 2, 2, BT, CW), BF16), vm((2, 2, 8, 128), F32),
                vm((GH, HW, FF), BF16), vm((GH, HW, FF), BF16),
                vm((NC, 2, 2, BT, CW), BF16), vm((NC, 2, BT, CW), BF16), vm((NC, 2, BT, CW), BF16), vm((NC, 2, BT, CW), BF16),
                vm((T, QW), BF16), vm((T, CW), BF16), vm((T, 128), F32), vm((T, 1), F32),
                vm((T, 128), F32), vm((NC, BT, CW), BF16),
                vm((D,), BF16), vm((D,), BF16), vm((QW,), BF16), vm((HEAD_DIM,), BF16), vm((HEAD_DIM,), BF16),
                vm((1, T), jnp.int32), vm((1, HEAD_DIM), F32),
            ] + sems,
            compiler_params=pltpu.CompilerParams(collective_id=0, has_side_effects=True, vmem_limit_bytes=67043328),
            name='layer',
        )(hidden, positions, gain_attn, w_q, b_q, w_k, b_k, w_v,
          b_v, w_o, gain_mlp, w_gate, w_up, w_down, freq)
        shapes = (jax.ShapeDtypeStruct((1, BT, D), BF16), jax.ShapeDtypeStruct((T, HEAD_DIM), BF16), jax.ShapeDtypeStruct((T, HEAD_DIM), BF16))
        out, kc, vc = pl.pallas_call(
            result_kernel,
            out_shape=shapes,
            in_specs=[pl.BlockSpec(memory_space=pl.ANY)] * 3,
            out_specs=(pl.BlockSpec(memory_space=pl.ANY),) * 3,
            scratch_shapes=[vm((NC, BT, CW), BF16), vm((2, T, HEAD_DIM), BF16), dma((NC + 2,)), dma((NC + 2,))],
            name='results',
        )(out, kc, vc)
        return out, kc.reshape(1, T, 1, HEAD_DIM), vc.reshape(1, T, 1, HEAD_DIM)

    token_rows = P('dp', 'tp', None)
    col_split = P(None, 'tp')
    row_split = P('tp', None)
    vec_split = P('tp')
    replicated = P(None)
    cache_spec = P('dp', None, 'tp', None)
    in_specs = (token_rows, P('dp', None), replicated, col_split, vec_split, col_split, vec_split, col_split, vec_split, row_split, replicated, col_split, col_split, row_split)
    out_specs = (token_rows, cache_spec, cache_spec)
    return jax.shard_map(local_layer, mesh=mesh, in_specs=in_specs, out_specs=out_specs, check_vma=False)
```

```python
import jax
import jax.numpy as jnp
import numpy as np
from jax import lax
from jax.experimental import pallas as pl
from jax.experimental.pallas import tpu as pltpu
from jax.sharding import PartitionSpec as P

HEAD_DIM = 128
ROPE_THETA = 1000000.0
NORM_EPS = 1e-6
D = 3584
HEADS = 7
QW = HEADS * HEAD_DIM
QKV = QW + 2 * HEAD_DIM
FF = 4736
NC = 7
CW = D // NC
BT = 64
T = 256
TW = 256
GH = 5
DS = 3
LATE = 3
HW = CW // 2
OUTS = ((0, 0, HW), (0, HW, HW)) + tuple((j, 0, CW) for j in range(1, NC - 1)) + ((NC - 1, 0, HW), (NC - 1, HW, HW))
NO = len(OUTS)
F32 = jnp.float32
BF16 = jnp.bfloat16
MESH = pl.DeviceIdType.MESH


def add(parts):
    first, second = parts
    return first + second


def dot(a, b):
    return jnp.dot(a, b, preferred_element_type=F32)


def row(ref, start, size):
    if not isinstance(start, int):
        start = pl.multiple_of(start, size)
    return ref[pl.ds(start, size)].astype(F32).reshape(1, size)


def result_kernel(out_i, kc_i, vc_i, out_o, kc_o, vc_o, outb, kb, vb, i_sem, o_sem):
    loads = [pltpu.make_async_copy(s, d, i_sem) for s, d in ((out_i, outb), (kc_i, kb), (vc_i, vb))]
    stores = [pltpu.make_async_copy(s, d, o_sem) for s, d in ((outb, out_o), (kb, kc_o), (vb, vc_o))]
    for cps in (loads, stores):
        for cp in cps:
            cp.start()
        for cp in cps:
            cp.wait()


def layer_kernel(x_h, pos_h, g1_h, wq_h, bq_h, wk_h, bk_h, wv_h, bv_h, wo_h, g2_h, wg_h, wu_h, wd_h, freq_h,
                 out_h, kc_h, vc_h,
                 xa, sta, gbuf, ubuf, pbuf, psib, sbuf, xs, obuf, hbuf, cprev, ssum, alpha, xs2,
                 g1, g2, bq, bk, bv, pos, freq,
                 sm_sem, x_sem, w_sem, wo_sem, g_sem, d_sem, o_sem, sent_x, sent_p, sent_o,
                 xp_r, xb_r, xf_r, st_r, ps_r, sx_r):
    tp = lax.axis_index('tp')
    c = lax.div(tp, 2)
    k = lax.rem(tp, 2)
    oc = 1 - c
    ok = 1 - k
    sib = 2 * c + ok
    par = 2 * oc + k

    def remote(src, dst, ssem, rsem, target):
        return pltpu.make_async_remote_copy(src_ref=src, dst_ref=dst, send_sem=ssem, recv_sem=rsem,
                                            device_id={'tp': target}, device_id_type=MESH)

    def x_load(j):
        return pltpu.make_async_copy(x_h.at[0, :, pl.ds(j * CW, CW)], xa.at[j, c, k], x_sem.at[min(j, 1)])

    for j in range(NC):
        x_load(j).start()
    small = [(g1_h, g1), (g2_h, g2), (bq_h, bq), (bk_h, bk), (bv_h, bv), (pos_h, pos), (freq_h, freq)]
    small_cp = [pltpu.make_async_copy(s, d, sm_sem) for i, (s, d) in enumerate(small)]
    for cp in small_cp:
        cp.start()

    def g_loads(i):
        slot = lax.rem(i, GH)
        rows = pl.ds(pl.multiple_of(i * HW, HW), HW)
        return (pltpu.make_async_copy(wg_h.at[rows], gbuf.at[slot], g_sem.at[slot]),
                pltpu.make_async_copy(wu_h.at[rows], ubuf.at[slot], g_sem.at[slot]))

    def attention_half(wb, wob, qkv):
        def w_loads(j):
            rows = pl.ds(j * CW, CW)
            return (pltpu.make_async_copy(wq_h.at[rows], wb.at[j, :, pl.ds(0, QW)], w_sem.at[j]),
                    pltpu.make_async_copy(wk_h.at[rows], wb.at[j, :, pl.ds(QW, HEAD_DIM)], w_sem.at[j]),
                    pltpu.make_async_copy(wv_h.at[rows], wb.at[j, :, pl.ds(QW + HEAD_DIM, HEAD_DIM)], w_sem.at[j]))

        for j in range(NC):
            for cp in w_loads(j):
                cp.start()
        wo_cp = pltpu.make_async_copy(wo_h, wob, wo_sem)
        wo_cp.start()
        for i in range(GH):
            for cp in g_loads(i):
                cp.start()

        barrier = pltpu.get_barrier_semaphore()
        for peer in (sib, par):
            pl.semaphore_signal(barrier, inc=1, device_id={'tp': peer}, device_id_type=MESH)
        pl.semaphore_wait(barrier, 2)

        def x_to_par(j):
            return remote(xa.at[j, c, k], xa.at[j, c, k], sent_x, xp_r.at[j], par)

        def x_from_par(j):
            return remote(xa.at[j, oc, k], xa.at[j, oc, k], sent_x, xp_r.at[j], par)

        def x_to_sib(j):
            return remote(xa.at[j, c, k], xa.at[j, c, k], sent_x, xb_r.at[j], sib)

        def x_from_sib(j):
            return remote(xa.at[j, c, ok], xa.at[j, c, ok], sent_x, xb_r.at[j], sib)

        def x_forward(j):
            return remote(xa.at[j, oc, k], xa.at[j, oc, k], sent_x, xf_r.at[j], sib)

        def x_forwarded(j):
            return remote(xa.at[j, oc, ok], xa.at[j, oc, ok], sent_x, xf_r.at[j], sib)

        x_load(0).wait()
        x_to_par(0).start()
        x_to_sib(0).start()
        for j in range(1, NC):
            x_load(j).wait()
        square = jnp.zeros((BT, CW), F32)
        for j in range(NC):
            part = xa[j, c, k].astype(F32)
            square = square + part * part
        mean = jnp.sum(square, axis=-1, keepdims=True) / D
        inv = jnp.broadcast_to(lax.rsqrt(mean + NORM_EPS), (BT, 128))
        sta[c, k] = jnp.transpose(jnp.concatenate([inv, inv], axis=0))[:8]
        st_par = remote(sta.at[c, k], sta.at[c, k], sent_x, st_r.at[0], par)
        st_par.start()
        st_sib = remote(sta.at[c, k], sta.at[c, k], sent_x, st_r.at[1], sib)
        st_sib.start()
        for j in range(1, NC):
            x_to_par(j).start()
            x_to_sib(j).start()

        for cp in small_cp:
            cp.wait()
        pos_col = jnp.transpose(jnp.broadcast_to(pos[...].astype(F32), (HEAD_DIM, T)))
        angles = pos_col * freq[...]
        cosine = jnp.cos(angles)
        sine = jnp.sin(angles)
        lane = lax.broadcasted_iota(jnp.int32, (T, HEAD_DIM), 1)
        sine = jnp.where(lane < HEAD_DIM // 2, -sine, sine)

        remote(sta.at[oc, k], sta.at[oc, k], sent_x, st_r.at[0], par).wait_recv()
        st_fwd = remote(sta.at[oc, k], sta.at[oc, k], sent_x, st_r.at[2], sib)
        st_fwd.start()
        remote(sta.at[c, ok], sta.at[c, ok], sent_x, st_r.at[1], sib).wait_recv()
        remote(sta.at[oc, ok], sta.at[oc, ok], sent_x, st_r.at[2], sib).wait_recv()
        for cc in range(2):
            for kk in range(2):
                wide = jnp.broadcast_to(sta[cc, kk][0:1], (128, 128))
                cprev[pl.ds((cc * 2 + kk) * BT, BT), :] = jnp.transpose(wide)[:BT]
        qkv[...] = jnp.zeros_like(qkv)

        def project(j):
            x_from_sib(j).wait_recv()
            x_forwarded(j).wait_recv()
            for cp in w_loads(j):
                cp.wait()
            values = xa[j].reshape(T, CW).astype(F32)
            scale = jnp.concatenate([cprev[...]] * (CW // 128), axis=1)
            gain = row(g1, j * CW, CW)
            hbuf[...] = (values * scale * gain).astype(BF16)
            qkv[...] += dot(hbuf[...], wb[j])

        x_from_par(0).wait_recv()
        x_forward(0).start()

        @pl.loop(1, NC)
        def _(j):
            x_from_par(j).wait_recv()
            x_forward(j).start()
            project(j - 1)

        project(NC - 1)

        def rotate(u, r):
            rows = slice(r * 2 * BT, (r + 1) * 2 * BT)
            return u * cosine[rows] + pltpu.roll(u, HEAD_DIM // 2, 1) * sine[rows]

        half = T // 2
        rows = HEADS * half
        row_i = lax.rem(lax.broadcasted_iota(jnp.int32, (rows, half), 0), half)
        causal = row_i >= lax.broadcasted_iota(jnp.int32, (rows, half), 1)
        key_lanes, value_lanes = pl.ds(0, HEAD_DIM), pl.ds(HEAD_DIM, HEAD_DIM)
        for r in range(2):
            width = half * (r + 1)
            part = pl.ds(r * half, half)
            hbuf[part, key_lanes] = rotate(qkv[part, pl.ds(QW, HEAD_DIM)] + row(bk, 0, HEAD_DIM), r).astype(BF16)
            hbuf[part, value_lanes] = (qkv[part, pl.ds(QW + HEAD_DIM, HEAD_DIM)] + row(bv, 0, HEAD_DIM)).astype(BF16)
            stacked = jnp.concatenate([
                rotate(qkv[part, pl.ds(h * HEAD_DIM, HEAD_DIM)] + row(bq, h * HEAD_DIM, HEAD_DIM), r).astype(BF16)
                for h in range(HEADS)], axis=0)
            scores = lax.dot_general(stacked, hbuf[pl.ds(0, width), key_lanes], (((1,), (1,)), ((), ())),
                                     preferred_element_type=F32) * (HEAD_DIM ** -0.5)
            last = jnp.where(causal, scores[:, width - half:], -1e30)
            scores = last if r == 0 else jnp.concatenate([scores[:, :half], last], axis=1)
            weights = jnp.exp(scores - jnp.max(scores, axis=-1, keepdims=True))
            probs = (weights * (1.0 / jnp.sum(weights, axis=-1, keepdims=True))).astype(BF16)
            out = dot(probs, hbuf[pl.ds(0, width), value_lanes]).astype(BF16)
            for h in range(HEADS):
                obuf[part, pl.ds(h * HEAD_DIM, HEAD_DIM)] = out[h * half:(h + 1) * half]
            if r == 0:
                wo_cp.wait()
            pbuf[0, r] = dot(obuf[part, :], wob[:, pl.ds(0, CW)]).astype(BF16).reshape(2, BT, CW)
            p_sends(0)[r].start()

        k_out = pltpu.make_async_copy(hbuf.at[:, key_lanes], kc_h, o_sem)
        v_out = pltpu.make_async_copy(hbuf.at[:, value_lanes], vc_h, o_sem)
        k_out.start()
        v_out.start()
        chip_partial(0, 0)
        lag = 3
        for j in range(1, NC):
            pbuf[j] = dot(obuf[...], wob[:, pl.ds(j * CW, CW)]).astype(BF16).reshape(2, 2, BT, CW)
            p_sends(j)[0].start()
            if j >= lag:
                chip_partial(j - lag, 1 if j == lag else 0)
        for j in range(NC - lag, NC):
            chip_partial(j, 0)

        @pl.loop(0, NC)
        def _(j):
            x_to_par(j).wait_send()
            x_to_sib(j).wait_send()
            x_forward(j).wait_send()

        st_par.wait_send()
        st_sib.wait_send()
        st_fwd.wait_send()
        k_out.wait()
        v_out.wait()

    def parts(j):
        if isinstance(j, int) and j == 0:
            return ((pl.ds(0, 1), 0), (pl.ds(1, 1), NC))
        return ((pl.ds(0, 2), j),)

    def p_sends(j):
        return [remote(pbuf.at[j, p, ok], psib.at[j, p], sent_p, ps_r.at[i], sib) for p, i in parts(j)]

    def s_sends(j):
        return [remote(sbuf.at[j, p], xs.at[j, p], sent_p, sx_r.at[i], par) for p, i in parts(j)]

    def chip_partial(j, which):
        p = parts(j)[which][0]
        p_sends(j)[which].wait_recv()
        sbuf[j, p] = (pbuf[j, p, k].astype(F32) + psib[j, p].astype(F32)).astype(BF16)
        s_sends(j)[which].start()

    pl.run_scoped(attention_half,
                  pltpu.VMEM((NC, CW, QKV), BF16), pltpu.VMEM((QW, D), BF16), pltpu.VMEM((T, QKV), F32))

    def mlp_half(accg, accu, act, dbuf):
        def d_load(j, slot):
            cols = pl.ds(pl.multiple_of(j * CW, CW), CW)
            return pltpu.make_async_copy(wd_h.at[:, cols], dbuf.at[slot], d_sem.at[slot])

        for s in range(DS):
            d_load(s, s).start()

        def x1_send(j):
            return remote(xa.at[j, :, k], xa.at[j, :, k], sent_o, xb_r.at[j], sib)

        def x1_recv(j):
            return remote(xa.at[j, :, ok], xa.at[j, :, ok], sent_o, xb_r.at[j], sib)

        def residual(j):
            for cp in s_sends(j):
                cp.wait_recv()
            total = sbuf[j].astype(F32) + xs[j].astype(F32)
            xa[j, :, k] = (xa[j, :, k].astype(F32) + total).astype(BF16)
            x1_send(j).start()

        def normalise(u):
            values = xa[u].reshape(T, CW).astype(F32)
            row_sum = jnp.sum(values * values, axis=-1, keepdims=True)
            first = isinstance(u, int) and u == 0
            if not first:
                row_sum = row_sum + ssum[...]
            ssum[...] = row_sum
            scale = lax.rsqrt(row_sum / ((u + 1) * CW) + NORM_EPS)
            wide = jnp.broadcast_to(scale, (T, 128))
            if not first:
                alpha[...] = wide / cprev[...]
            cprev[...] = wide
            hbuf[...] = (values * scale * row(g2, u * CW, CW)).astype(BF16)

        def put(mode, rows, cols, dg, du):
            w = dg.shape[1]
            if mode != 'first':
                al = jnp.concatenate([alpha[rows, :]] * (w // 128), axis=1)
                dg = accg[rows, cols] * al + dg
                du = accu[rows, cols] * al + du
            if mode == 'last':
                act[rows, cols] = (dg / (1.0 + jnp.exp(-dg)) * du).astype(BF16)
            else:
                accg[rows, cols] = dg
                accu[rows, cols] = du

        def tiles(halves, mode, lo, hi):
            for n in range(lo, hi):
                cols = pl.ds(n * TW, TW)
                dg, du = [add([dot(hbuf[:, pl.ds(i * HW, HW)], ref[slot, :, cols]) for i, slot in enumerate(halves)])
                          for ref in (gbuf, ubuf)]
                put(mode, pl.ds(0, T), cols, dg, du)

        def tail(halves, mode):
            cols = pl.ds(FF - 128, 128)
            weight = [jnp.concatenate([gbuf[slot, :, cols], ubuf[slot, :, cols]], axis=1) for slot in halves]
            for r in range(2):
                rows = pl.ds(r * 2 * BT, 2 * BT)
                res = add([dot(hbuf[rows, pl.ds(i * HW, HW)], w) for i, w in enumerate(weight)])
                put(mode, rows, cols, res[:, :128], res[:, 128:])

        NT = FF // TW

        def gate_up(u, mode, cut):
            x1_recv(u).wait_recv()
            for i in range(2):
                for cp in g_loads(2 * u + i):
                    cp.wait()
            halves = [lax.rem(2 * u + i, GH) for i in range(2)]
            if cut == 0:
                residual(u + 1)
            normalise(u)
            if mode == 'last':
                tiles(halves, mode, 0, NT)
            else:
                tiles(halves, mode, 0, cut)
                if cut:
                    residual(u + 1)
                tiles(halves, mode, cut, NT)
            tail(halves, mode)

        def refill(i):
            for cp in g_loads(i):
                cp.start()

        residual(0)
        gate_up(0, 'first', 13)
        for i in range(2):
            refill(GH + i)

        def middle(u, cut):
            gate_up(u, 'mid', cut)
            for i in range(2):
                @pl.when(2 * u + i + GH < 2 * NC)
                def _():
                    refill(2 * u + i + GH)

        pl.loop(1, LATE)(lambda u: middle(u, 9))
        pl.loop(LATE, NC - 1)(lambda u: middle(u, 0))
        gate_up(NC - 1, 'last', NT)

        for j in range(NC):
            for cp in p_sends(j) + s_sends(j):
                cp.wait_send()

        def p2_send(u, j, lo, w):
            lanes = pl.ds(lo, w)
            return remote(pbuf.at[j, :, ok, :, lanes], psib.at[j, :, :, lanes], sent_o, ps_r.at[u], sib)

        def s2_send(u, j, lo, w):
            lanes = pl.ds(lo, w)
            return remote(sbuf.at[j, oc, :, lanes], xs2.at[j, :, lanes], sent_o, xp_r.at[u], par)

        def out_copy(u, j, lo, w):
            start = j * CW + lo
            cols = pl.ds(start if isinstance(start, int) else pl.multiple_of(start, CW), w)
            return pltpu.make_async_copy(sbuf.at[j, c, :, pl.ds(lo, w)], out_h.at[0, :, cols], o_sem)

        def down(u, j, lo, w):
            slot = lax.rem(j, DS)
            lanes = pl.ds(lo, w)
            if lo == 0:
                d_load(j, slot).wait()
            if w == CW:
                pbuf[j] = dot(act[...], dbuf[slot]).astype(BF16).reshape(2, 2, BT, w)
            else:
                for r in range(2):
                    part = dot(act[pl.ds(r * 2 * BT, 2 * BT), :], dbuf[slot, :, lanes])
                    pbuf[j, r, :, :, lanes] = part.astype(BF16).reshape(2, BT, w)
            p2_send(u, j, lo, w).start()

        def chip_sum(u, j, lo, w):
            lanes = pl.ds(lo, w)
            p2_send(u, j, lo, w).wait_recv()
            sbuf[j, oc, :, lanes] = (pbuf[j, oc, k, :, lanes].astype(F32) + psib[j, oc, :, lanes].astype(F32)).astype(BF16)
            s2_send(u, j, lo, w).start()

        def finish(u, j, lo, w):
            lanes = pl.ds(lo, w)
            s2_send(u, j, lo, w).wait_recv()
            total = pbuf[j, c, k, :, lanes].astype(F32) + psib[j, c, :, lanes].astype(F32) + xs2[j, :, lanes].astype(F32)
            sbuf[j, c, :, lanes] = (xa[j, c, k, :, lanes].astype(F32) + total).astype(BF16)
            out_copy(u, j, lo, w).start()

        outs = [(u,) + OUTS[u] for u in range(NO)]

        down(*outs[0])
        down(*outs[1])
        d_load(DS, 0).start()
        chip_sum(*outs[0])

        @pl.loop(1, NC - 1)
        def _(j):
            down(j + 1, j, 0, CW)

            @pl.when(j + DS < NC)
            def _():
                d_load(j + DS, lax.rem(j, DS)).start()

            @pl.when(j == 1)
            def _():
                chip_sum(*outs[1])

            @pl.when(j > 1)
            def _():
                chip_sum(j, j - 1, 0, CW)

        down(*outs[NO - 2])
        chip_sum(*outs[NO - 3])
        down(*outs[NO - 1])
        chip_sum(*outs[NO - 2])
        for u in range(NO - 4):
            finish(*outs[u])
        chip_sum(*outs[NO - 1])
        for u in range(NO - 4, NO):
            finish(*outs[u])

        for j in range(NC):
            x1_send(j).wait_send()
        for u in range(NO):
            p2_send(*outs[u]).wait_send()
            s2_send(*outs[u]).wait_send()
            out_copy(*outs[u]).wait()

    pl.run_scoped(mlp_half,
                  pltpu.VMEM((T, FF), F32), pltpu.VMEM((T, FF), F32), pltpu.VMEM((T, FF), BF16),
                  pltpu.VMEM((DS, FF, CW), BF16))


def solution(mesh):
    def local_layer(hidden, positions, gain_attn, w_q, b_q, w_k, b_k, w_v, b_v, w_o, gain_mlp, w_gate, w_up, w_down):
        half = HEAD_DIM // 2
        freq = ROPE_THETA ** (-np.arange(half) / half)
        freq = np.concatenate([freq, freq]).reshape(1, HEAD_DIM).astype(np.float32)
        dma = pltpu.SemaphoreType.DMA
        sems = [dma, dma((2,)), dma((NC,)), dma, dma((GH,)), dma((DS,)), dma, dma, dma, dma,
                dma((NO,)), dma((NC,)), dma((NC,)), dma((3,)), dma((NO,)), dma((NC + 1,))]
        vm = pltpu.VMEM
        out, kc, vc = pl.pallas_call(
            layer_kernel,
            out_shape=(jax.ShapeDtypeStruct((1, BT, D), BF16), jax.ShapeDtypeStruct((T, HEAD_DIM), BF16),
                       jax.ShapeDtypeStruct((T, HEAD_DIM), BF16)),
            in_specs=[pl.BlockSpec(memory_space=pl.ANY)] * 15,
            out_specs=(pl.BlockSpec(memory_space=pl.ANY),) * 3,
            scratch_shapes=[
                vm((NC, 2, 2, BT, CW), BF16), vm((2, 2, 8, 128), F32),
                vm((GH, HW, FF), BF16), vm((GH, HW, FF), BF16),
                vm((NC, 2, 2, BT, CW), BF16), vm((NC, 2, BT, CW), BF16), vm((NC, 2, BT, CW), BF16), vm((NC, 2, BT, CW), BF16),
                vm((T, QW), BF16), vm((T, CW), BF16), vm((T, 128), F32), vm((T, 1), F32),
                vm((T, 128), F32), vm((NC, BT, CW), BF16),
                vm((D,), BF16), vm((D,), BF16), vm((QW,), BF16), vm((HEAD_DIM,), BF16), vm((HEAD_DIM,), BF16),
                vm((1, T), jnp.int32), vm((1, HEAD_DIM), F32),
            ] + sems,
            compiler_params=pltpu.CompilerParams(collective_id=0, has_side_effects=True, vmem_limit_bytes=67043328),
            name='layer',
        )(hidden, positions, gain_attn, w_q, b_q, w_k, b_k, w_v,
          b_v, w_o, gain_mlp, w_gate, w_up, w_down, freq)
        shapes = (jax.ShapeDtypeStruct((1, BT, D), BF16), jax.ShapeDtypeStruct((T, HEAD_DIM), BF16), jax.ShapeDtypeStruct((T, HEAD_DIM), BF16))
        out, kc, vc = pl.pallas_call(
            result_kernel,
            out_shape=shapes,
            in_specs=[pl.BlockSpec(memory_space=pl.ANY)] * 3,
            out_specs=(pl.BlockSpec(memory_space=pl.ANY),) * 3,
            scratch_shapes=[vm((1, BT, D), BF16), vm((T, HEAD_DIM), BF16), vm((T, HEAD_DIM), BF16), dma, dma],
            name='results',
        )(out, kc, vc)
        return out, kc.reshape(1, T, 1, HEAD_DIM), vc.reshape(1, T, 1, HEAD_DIM)

    token_rows = P('dp', 'tp', None)
    col_split = P(None, 'tp')
    row_split = P('tp', None)
    vec_split = P('tp')
    replicated = P(None)
    cache_spec = P('dp', None, 'tp', None)
    in_specs = (token_rows, P('dp', None), replicated, col_split, vec_split, col_split, vec_split, col_split, vec_split, row_split, replicated, col_split, col_split, row_split)
    out_specs = (token_rows, cache_spec, cache_spec)
    return jax.shard_map(local_layer, mesh=mesh, in_specs=in_specs, out_specs=out_specs, check_vma=False)
```

```python
import jax
import jax.numpy as jnp
import numpy as np
from jax import lax
from jax.experimental import pallas as pl
from jax.experimental.pallas import tpu as pltpu
from jax.sharding import PartitionSpec as P

HEAD_DIM = 128
ROPE_THETA = 1000000.0
NORM_EPS = 1e-6
D = 3584
HEADS = 7
QW = HEADS * HEAD_DIM
QKV = QW + 2 * HEAD_DIM
FF = 4736
NC = 7
CW = D // NC
BT = 64
T = 256
TW = 256
GH = 5
DS = 3
LATE = 3
HW = CW // 2
NO = NC + 2
SPLIT = NC - 2
F32 = jnp.float32
BF16 = jnp.bfloat16
MESH = pl.DeviceIdType.MESH


def add(parts):
    first, second = parts
    return first + second


def dot(a, b):
    return jnp.dot(a, b, preferred_element_type=F32)


def row(ref, start, size):
    if not isinstance(start, int):
        start = pl.multiple_of(start, size)
    return ref[pl.ds(start, size)].astype(F32).reshape(1, size)


def result_kernel(out_i, kc_i, vc_i, out_o, kc_o, vc_o, outb, kb, vb, i_sem, o_sem):
    loads = [pltpu.make_async_copy(s, d, i_sem) for s, d in ((out_i, outb), (kc_i, kb), (vc_i, vb))]
    stores = [pltpu.make_async_copy(s, d, o_sem) for s, d in ((outb, out_o), (kb, kc_o), (vb, vc_o))]
    for cps in (loads, stores):
        for cp in cps:
            cp.start()
        for cp in cps:
            cp.wait()


def layer_kernel(x_h, pos_h, g1_h, wq_h, bq_h, wk_h, bk_h, wv_h, bv_h, wo_h, g2_h, wg_h, wu_h, wd_h, freq_h,
                 out_h, kc_h, vc_h,
                 xa, sta, gbuf, ubuf, pbuf, psib, sbuf, xs, obuf, hbuf, cprev, ssum, alpha, xs2,
                 g1, g2, bq, bk, bv, pos, freq,
                 sm_sem, x_sem, w_sem, wo_sem, g_sem, d_sem, o_sem, sent_x, sent_p, sent_o,
                 xp_r, xb_r, xf_r, st_r, ps_r, sx_r):
    tp = lax.axis_index('tp')
    c = lax.div(tp, 2)
    k = lax.rem(tp, 2)
    oc = 1 - c
    ok = 1 - k
    sib = 2 * c + ok
    par = 2 * oc + k

    def remote(src, dst, ssem, rsem, target):
        return pltpu.make_async_remote_copy(src_ref=src, dst_ref=dst, send_sem=ssem, recv_sem=rsem,
                                            device_id={'tp': target}, device_id_type=MESH)

    def x_load(j):
        return pltpu.make_async_copy(x_h.at[0, :, pl.ds(j * CW, CW)], xa.at[j, c, k], x_sem.at[min(j, 1)])

    for j in range(NC):
        x_load(j).start()
    small = [(g1_h, g1), (g2_h, g2), (bq_h, bq), (bk_h, bk), (bv_h, bv), (pos_h, pos), (freq_h, freq)]
    small_cp = [pltpu.make_async_copy(s, d, sm_sem) for i, (s, d) in enumerate(small)]
    for cp in small_cp:
        cp.start()

    def g_loads(i):
        slot = lax.rem(i, GH)
        rows = pl.ds(pl.multiple_of(i * HW, HW), HW)
        return (pltpu.make_async_copy(wg_h.at[rows], gbuf.at[slot], g_sem.at[slot]),
                pltpu.make_async_copy(wu_h.at[rows], ubuf.at[slot], g_sem.at[slot]))

    def attention_half(wb, wob, qkv):
        def w_loads(j):
            rows = pl.ds(j * CW, CW)
            return (pltpu.make_async_copy(wq_h.at[rows], wb.at[j, :, pl.ds(0, QW)], w_sem.at[j]),
                    pltpu.make_async_copy(wk_h.at[rows], wb.at[j, :, pl.ds(QW, HEAD_DIM)], w_sem.at[j]),
                    pltpu.make_async_copy(wv_h.at[rows], wb.at[j, :, pl.ds(QW + HEAD_DIM, HEAD_DIM)], w_sem.at[j]))

        for j in range(NC):
            for cp in w_loads(j):
                cp.start()
        wo_cp = pltpu.make_async_copy(wo_h, wob, wo_sem)
        wo_cp.start()
        for i in range(GH):
            for cp in g_loads(i):
                cp.start()

        barrier = pltpu.get_barrier_semaphore()
        for peer in (sib, par):
            pl.semaphore_signal(barrier, inc=1, device_id={'tp': peer}, device_id_type=MESH)
        pl.semaphore_wait(barrier, 2)

        def x_to_par(j):
            return remote(xa.at[j, c, k], xa.at[j, c, k], sent_x, xp_r.at[j], par)

        def x_from_par(j):
            return remote(xa.at[j, oc, k], xa.at[j, oc, k], sent_x, xp_r.at[j], par)

        def x_to_sib(j):
            return remote(xa.at[j, c, k], xa.at[j, c, k], sent_x, xb_r.at[j], sib)

        def x_from_sib(j):
            return remote(xa.at[j, c, ok], xa.at[j, c, ok], sent_x, xb_r.at[j], sib)

        def x_forward(j):
            return remote(xa.at[j, oc, k], xa.at[j, oc, k], sent_x, xf_r.at[j], sib)

        def x_forwarded(j):
            return remote(xa.at[j, oc, ok], xa.at[j, oc, ok], sent_x, xf_r.at[j], sib)

        x_load(0).wait()
        x_to_par(0).start()
        x_to_sib(0).start()
        for j in range(1, NC):
            x_load(j).wait()
        square = jnp.zeros((BT, CW), F32)
        for j in range(NC):
            part = xa[j, c, k].astype(F32)
            square = square + part * part
        mean = jnp.sum(square, axis=-1, keepdims=True) / D
        inv = jnp.broadcast_to(lax.rsqrt(mean + NORM_EPS), (BT, 128))
        sta[c, k] = jnp.transpose(jnp.concatenate([inv, inv], axis=0))[:8]
        st_par = remote(sta.at[c, k], sta.at[c, k], sent_x, st_r.at[0], par)
        st_par.start()
        st_sib = remote(sta.at[c, k], sta.at[c, k], sent_x, st_r.at[1], sib)
        st_sib.start()
        for j in range(1, NC):
            x_to_par(j).start()
            x_to_sib(j).start()

        for cp in small_cp:
            cp.wait()
        pos_col = jnp.transpose(jnp.broadcast_to(pos[...].astype(F32), (HEAD_DIM, T)))
        angles = pos_col * freq[...]
        cosine = jnp.cos(angles)
        sine = jnp.sin(angles)
        lane = lax.broadcasted_iota(jnp.int32, (T, HEAD_DIM), 1)
        sine = jnp.where(lane < HEAD_DIM // 2, -sine, sine)

        remote(sta.at[oc, k], sta.at[oc, k], sent_x, st_r.at[0], par).wait_recv()
        st_fwd = remote(sta.at[oc, k], sta.at[oc, k], sent_x, st_r.at[2], sib)
        st_fwd.start()
        remote(sta.at[c, ok], sta.at[c, ok], sent_x, st_r.at[1], sib).wait_recv()
        remote(sta.at[oc, ok], sta.at[oc, ok], sent_x, st_r.at[2], sib).wait_recv()
        for cc in range(2):
            for kk in range(2):
                wide = jnp.broadcast_to(sta[cc, kk][0:1], (128, 128))
                cprev[pl.ds((cc * 2 + kk) * BT, BT), :] = jnp.transpose(wide)[:BT]
        qkv[...] = jnp.zeros_like(qkv)

        def project(j):
            x_from_sib(j).wait_recv()
            x_forwarded(j).wait_recv()
            for cp in w_loads(j):
                cp.wait()
            values = xa[j].reshape(T, CW).astype(F32)
            scale = jnp.concatenate([cprev[...]] * (CW // 128), axis=1)
            gain = row(g1, j * CW, CW)
            hbuf[...] = (values * scale * gain).astype(BF16)
            qkv[...] += dot(hbuf[...], wb[j])

        x_from_par(0).wait_recv()
        x_forward(0).start()

        @pl.loop(1, NC)
        def _(j):
            x_from_par(j).wait_recv()
            x_forward(j).start()
            project(j - 1)

        project(NC - 1)

        def rotate(u, r):
            rows = slice(r * 2 * BT, (r + 1) * 2 * BT)
            return u * cosine[rows] + pltpu.roll(u, HEAD_DIM // 2, 1) * sine[rows]

        half = T // 2
        rows = 4 * half
        row_i = lax.rem(lax.broadcasted_iota(jnp.int32, (rows, half), 0), half)
        causal = row_i >= lax.broadcasted_iota(jnp.int32, (rows, half), 1)
        key_lanes, value_lanes = pl.ds(0, HEAD_DIM), pl.ds(HEAD_DIM, HEAD_DIM)
        for r in range(2):
            width = half * (r + 1)
            part = pl.ds(r * half, half)
            hbuf[part, key_lanes] = rotate(qkv[part, pl.ds(QW, HEAD_DIM)] + row(bk, 0, HEAD_DIM), r).astype(BF16)
            hbuf[part, value_lanes] = (qkv[part, pl.ds(QW + HEAD_DIM, HEAD_DIM)] + row(bv, 0, HEAD_DIM)).astype(BF16)
            for heads in (range(4), range(4, HEADS)):
                stacked = jnp.concatenate([
                    rotate(qkv[part, pl.ds(h * HEAD_DIM, HEAD_DIM)] + row(bq, h * HEAD_DIM, HEAD_DIM), r).astype(BF16)
                    for h in heads], axis=0)
                scores = lax.dot_general(stacked, hbuf[pl.ds(0, width), key_lanes], (((1,), (1,)), ((), ())),
                                         preferred_element_type=F32) * (HEAD_DIM ** -0.5)
                last = jnp.where(causal[:len(heads) * half], scores[:, width - half:], -1e30)
                scores = last if r == 0 else jnp.concatenate([scores[:, :half], last], axis=1)
                weights = jnp.exp(scores - jnp.max(scores, axis=-1, keepdims=True))
                probs = (weights * (1.0 / jnp.sum(weights, axis=-1, keepdims=True))).astype(BF16)
                out = dot(probs, hbuf[pl.ds(0, width), value_lanes]).astype(BF16)
                for i, h in enumerate(heads):
                    obuf[part, pl.ds(h * HEAD_DIM, HEAD_DIM)] = out[i * half:(i + 1) * half]
            if r == 0:
                wo_cp.wait()
            pbuf[0, r] = dot(obuf[part, :], wob[:, pl.ds(0, CW)]).astype(BF16).reshape(2, BT, CW)
            p_sends(0)[r].start()

        k_out = pltpu.make_async_copy(hbuf.at[:, key_lanes], kc_h, o_sem)
        v_out = pltpu.make_async_copy(hbuf.at[:, value_lanes], vc_h, o_sem)
        k_out.start()
        v_out.start()
        chip_partial(0, 0)
        lag = 3
        for j in range(1, NC):
            pbuf[j] = dot(obuf[...], wob[:, pl.ds(j * CW, CW)]).astype(BF16).reshape(2, 2, BT, CW)
            p_sends(j)[0].start()
            if j >= lag:
                chip_partial(j - lag, 1 if j == lag else 0)
        for j in range(NC - lag, NC):
            chip_partial(j, 0)

        @pl.loop(0, NC)
        def _(j):
            x_to_par(j).wait_send()
            x_to_sib(j).wait_send()
            x_forward(j).wait_send()

        st_par.wait_send()
        st_sib.wait_send()
        st_fwd.wait_send()
        k_out.wait()
        v_out.wait()

    def parts(j):
        if isinstance(j, int) and j == 0:
            return ((pl.ds(0, 1), 0), (pl.ds(1, 1), NC))
        return ((pl.ds(0, 2), j),)

    def p_sends(j):
        return [remote(pbuf.at[j, p, ok], psib.at[j, p], sent_p, ps_r.at[i], sib) for p, i in parts(j)]

    def s_sends(j):
        return [remote(sbuf.at[j, p], xs.at[j, p], sent_p, sx_r.at[i], par) for p, i in parts(j)]

    def chip_partial(j, which):
        p = parts(j)[which][0]
        p_sends(j)[which].wait_recv()
        sbuf[j, p] = (pbuf[j, p, k].astype(F32) + psib[j, p].astype(F32)).astype(BF16)
        s_sends(j)[which].start()

    pl.run_scoped(attention_half,
                  pltpu.VMEM((NC, CW, QKV), BF16), pltpu.VMEM((QW, D), BF16), pltpu.VMEM((T, QKV), F32))

    def mlp_half(accg, accu, act, dbuf):
        def d_load(j, slot):
            cols = pl.ds(pl.multiple_of(j * CW, CW), CW)
            return pltpu.make_async_copy(wd_h.at[:, cols], dbuf.at[slot], d_sem.at[slot])

        for s in range(DS):
            d_load(s, s).start()

        def x1_send(j):
            return remote(xa.at[j, :, k], xa.at[j, :, k], sent_o, xb_r.at[j], sib)

        def x1_recv(j):
            return remote(xa.at[j, :, ok], xa.at[j, :, ok], sent_o, xb_r.at[j], sib)

        def residual(j):
            for cp in s_sends(j):
                cp.wait_recv()
            total = sbuf[j].astype(F32) + xs[j].astype(F32)
            xa[j, :, k] = (xa[j, :, k].astype(F32) + total).astype(BF16)
            x1_send(j).start()

        def normalise(u):
            values = xa[u].reshape(T, CW).astype(F32)
            row_sum = jnp.sum(values * values, axis=-1, keepdims=True)
            first = isinstance(u, int) and u == 0
            if not first:
                row_sum = row_sum + ssum[...]
            ssum[...] = row_sum
            scale = lax.rsqrt(row_sum / ((u + 1) * CW) + NORM_EPS)
            wide = jnp.broadcast_to(scale, (T, 128))
            if not first:
                alpha[...] = wide / cprev[...]
            cprev[...] = wide
            hbuf[...] = (values * scale * row(g2, u * CW, CW)).astype(BF16)

        def put(mode, rows, cols, dg, du):
            w = dg.shape[1]
            if mode != 'first':
                al = jnp.concatenate([alpha[rows, :]] * (w // 128), axis=1)
                dg = accg[rows, cols] * al + dg
                du = accu[rows, cols] * al + du
            if mode == 'last':
                act[rows, cols] = (dg / (1.0 + jnp.exp(-dg)) * du).astype(BF16)
            else:
                accg[rows, cols] = dg
                accu[rows, cols] = du

        def tiles(halves, mode, lo, hi):
            for n in range(lo, hi):
                cols = pl.ds(n * TW, TW)
                dg, du = [add([dot(hbuf[:, pl.ds(i * HW, HW)], ref[slot, :, cols]) for i, slot in enumerate(halves)])
                          for ref in (gbuf, ubuf)]
                put(mode, pl.ds(0, T), cols, dg, du)

        def tail(halves, mode):
            cols = pl.ds(FF - 128, 128)
            weight = [jnp.concatenate([gbuf[slot, :, cols], ubuf[slot, :, cols]], axis=1) for slot in halves]
            for r in range(2):
                rows = pl.ds(r * 2 * BT, 2 * BT)
                res = add([dot(hbuf[rows, pl.ds(i * HW, HW)], w) for i, w in enumerate(weight)])
                put(mode, rows, cols, res[:, :128], res[:, 128:])

        NT = FF // TW

        def gate_up(u, mode, cut):
            x1_recv(u).wait_recv()
            for i in range(2):
                for cp in g_loads(2 * u + i):
                    cp.wait()
            halves = [lax.rem(2 * u + i, GH) for i in range(2)]
            if cut == 0:
                residual(u + 1)
            normalise(u)
            if mode == 'last':
                tiles(halves, mode, 0, NT)
            else:
                tiles(halves, mode, 0, cut)
                if cut:
                    residual(u + 1)
                tiles(halves, mode, cut, NT)
            tail(halves, mode)

        def refill(i):
            for cp in g_loads(i):
                cp.start()

        residual(0)
        gate_up(0, 'first', 13)
        for i in range(2):
            refill(GH + i)

        def middle(u, cut):
            gate_up(u, 'mid', cut)
            for i in range(2):
                @pl.when(2 * u + i + GH < 2 * NC)
                def _():
                    refill(2 * u + i + GH)

        pl.loop(1, LATE)(lambda u: middle(u, 9))
        pl.loop(LATE, NC - 1)(lambda u: middle(u, 0))
        gate_up(NC - 1, 'last', NT)

        for j in range(NC):
            for cp in p_sends(j) + s_sends(j):
                cp.wait_send()

        def p2_send(j):
            return remote(pbuf.at[j, :, ok], psib.at[j], sent_o, ps_r.at[j], sib)

        def p2_block(j, block, sem):
            return remote(pbuf.at[j, block, ok], psib.at[j, block], sent_o, ps_r.at[sem], sib)

        def s2_send(j):
            return remote(sbuf.at[j, oc], xs2.at[j], sent_o, xp_r.at[j], par)

        def out_copy(j):
            return pltpu.make_async_copy(sbuf.at[j, c], out_h.at[0, :, pl.ds(pl.multiple_of(j * CW, CW), CW)], o_sem)

        def down(j):
            slot = lax.rem(j, DS)
            d_load(j, slot).wait()
            pbuf[j] = dot(act[...], dbuf[slot]).astype(BF16).reshape(2, 2, BT, CW)
            p2_send(j).start()

        def down_rows(j, block, sem):
            rows = pl.ds(pl.multiple_of(block * 2 * BT, 2 * BT), 2 * BT)
            pbuf[j, block] = dot(act[rows, :], dbuf[j % DS]).astype(BF16).reshape(2, BT, CW)
            p2_block(j, block, sem).start()

        def chip_sum(j, recv):
            recv.wait_recv()
            sbuf[j, oc] = (pbuf[j, oc, k].astype(F32) + psib[j, oc].astype(F32)).astype(BF16)
            s2_send(j).start()

        def finish(j):
            s2_send(j).wait_recv()
            total = pbuf[j, c, k].astype(F32) + psib[j, c].astype(F32) + xs2[j].astype(F32)
            sbuf[j, c] = (xa[j, c, k].astype(F32) + total).astype(BF16)
            out_copy(j).start()

        down(0)
        d_load(DS, 0).start()

        @pl.loop(1, SPLIT)
        def _(j):
            down(j)

            @pl.when(j + DS < NC)
            def _():
                d_load(j + DS, lax.rem(j, DS)).start()

            chip_sum(j - 1, p2_send(j - 1))

        one, two = SPLIT, SPLIT + 1
        d_load(one, one % DS).wait()
        down_rows(one, oc, one)
        chip_sum(one - 1, p2_send(one - 1))
        d_load(two, two % DS).wait()
        down_rows(two, oc, two)
        chip_sum(one, p2_block(one, oc, one))
        down_rows(one, c, NC)
        chip_sum(two, p2_block(two, oc, two))
        down_rows(two, c, NC + 1)
        pl.loop(0, SPLIT)(finish)
        p2_block(one, c, NC).wait_recv()
        finish(one)
        p2_block(two, c, NC + 1).wait_recv()
        finish(two)

        for j in range(NC):
            x1_send(j).wait_send()
            p2_send(j).wait_send()
            s2_send(j).wait_send()
            out_copy(j).wait()

    pl.run_scoped(mlp_half,
                  pltpu.VMEM((T, FF), F32), pltpu.VMEM((T, FF), F32), pltpu.VMEM((T, FF), BF16),
                  pltpu.VMEM((DS, FF, CW), BF16))


def solution(mesh):
    def local_layer(hidden, positions, gain_attn, w_q, b_q, w_k, b_k, w_v, b_v, w_o, gain_mlp, w_gate, w_up, w_down):
        half = HEAD_DIM // 2
        freq = ROPE_THETA ** (-np.arange(half) / half)
        freq = np.concatenate([freq, freq]).reshape(1, HEAD_DIM).astype(np.float32)
        dma = pltpu.SemaphoreType.DMA
        sems = [dma, dma((2,)), dma((NC,)), dma, dma((GH,)), dma((DS,)), dma, dma, dma, dma,
                dma((NO,)), dma((NC,)), dma((NC,)), dma((3,)), dma((NO,)), dma((NC + 1,))]
        vm = pltpu.VMEM
        out, kc, vc = pl.pallas_call(
            layer_kernel,
            out_shape=(jax.ShapeDtypeStruct((1, BT, D), BF16), jax.ShapeDtypeStruct((T, HEAD_DIM), BF16),
                       jax.ShapeDtypeStruct((T, HEAD_DIM), BF16)),
            in_specs=[pl.BlockSpec(memory_space=pl.ANY)] * 15,
            out_specs=(pl.BlockSpec(memory_space=pl.ANY),) * 3,
            scratch_shapes=[
                vm((NC, 2, 2, BT, CW), BF16), vm((2, 2, 8, 128), F32),
                vm((GH, HW, FF), BF16), vm((GH, HW, FF), BF16),
                vm((NC, 2, 2, BT, CW), BF16), vm((NC, 2, BT, CW), BF16), vm((NC, 2, BT, CW), BF16), vm((NC, 2, BT, CW), BF16),
                vm((T, QW), BF16), vm((T, CW), BF16), vm((T, 128), F32), vm((T, 1), F32),
                vm((T, 128), F32), vm((NC, BT, CW), BF16),
                vm((D,), BF16), vm((D,), BF16), vm((QW,), BF16), vm((HEAD_DIM,), BF16), vm((HEAD_DIM,), BF16),
                vm((1, T), jnp.int32), vm((1, HEAD_DIM), F32),
            ] + sems,
            compiler_params=pltpu.CompilerParams(collective_id=0, has_side_effects=True, vmem_limit_bytes=67043328),
            name='layer',
        )(hidden, positions, gain_attn, w_q, b_q, w_k, b_k, w_v,
          b_v, w_o, gain_mlp, w_gate, w_up, w_down, freq)
        shapes = (jax.ShapeDtypeStruct((1, BT, D), BF16), jax.ShapeDtypeStruct((T, HEAD_DIM), BF16), jax.ShapeDtypeStruct((T, HEAD_DIM), BF16))
        out, kc, vc = pl.pallas_call(
            result_kernel,
            out_shape=shapes,
            in_specs=[pl.BlockSpec(memory_space=pl.ANY)] * 3,
            out_specs=(pl.BlockSpec(memory_space=pl.ANY),) * 3,
            scratch_shapes=[vm((1, BT, D), BF16), vm((T, HEAD_DIM), BF16), vm((T, HEAD_DIM), BF16), dma, dma],
            name='results',
        )(out, kc, vc)
        return out, kc.reshape(1, T, 1, HEAD_DIM), vc.reshape(1, T, 1, HEAD_DIM)

    token_rows = P('dp', 'tp', None)
    col_split = P(None, 'tp')
    row_split = P('tp', None)
    vec_split = P('tp')
    replicated = P(None)
    cache_spec = P('dp', None, 'tp', None)
    in_specs = (token_rows, P('dp', None), replicated, col_split, vec_split, col_split, vec_split, col_split, vec_split, row_split, replicated, col_split, col_split, row_split)
    out_specs = (token_rows, cache_spec, cache_spec)
    return jax.shard_map(local_layer, mesh=mesh, in_specs=in_specs, out_specs=out_specs, check_vma=False)
```

```python
import jax
import jax.numpy as jnp
import numpy as np
from jax import lax
from jax.experimental import pallas as pl
from jax.experimental.pallas import tpu as pltpu
from jax.sharding import PartitionSpec as P

HEAD_DIM = 128
ROPE_THETA = 1000000.0
NORM_EPS = 1e-6
D = 3584
HEADS = 7
QW = HEADS * HEAD_DIM
QKV = QW + 2 * HEAD_DIM
FF = 4736
NC = 7
CW = D // NC
BT = 64
T = 256
TW = 256
GH = 5
DS = 3
LATE = 4
HW = CW // 2
NO = NC + 2
SPLIT = NC - 2
F32 = jnp.float32
BF16 = jnp.bfloat16
MESH = pl.DeviceIdType.MESH


def add(parts):
    first, second = parts
    return first + second


def dot(a, b):
    return jnp.dot(a, b, preferred_element_type=F32)


def row(ref, start, size):
    if not isinstance(start, int):
        start = pl.multiple_of(start, size)
    return ref[pl.ds(start, size)].astype(F32).reshape(1, size)


def result_kernel(out_i, kc_i, vc_i, out_o, kc_o, vc_o, outb, kb, vb, i_sem, o_sem):
    loads = [pltpu.make_async_copy(s, d, i_sem) for s, d in ((out_i, outb), (kc_i, kb), (vc_i, vb))]
    stores = [pltpu.make_async_copy(s, d, o_sem) for s, d in ((outb, out_o), (kb, kc_o), (vb, vc_o))]
    for cps in (loads, stores):
        for cp in cps:
            cp.start()
        for cp in cps:
            cp.wait()


def layer_kernel(x_h, pos_h, g1_h, wq_h, bq_h, wk_h, bk_h, wv_h, bv_h, wo_h, g2_h, wg_h, wu_h, wd_h, freq_h,
                 out_h, kc_h, vc_h,
                 xa, sta, gbuf, ubuf, pbuf, psib, sbuf, xs, obuf, hbuf, cprev, ssum, alpha, xs2,
                 g1, g2, bq, bk, bv, pos, freq,
                 sm_sem, x_sem, w_sem, wo_sem, g_sem, d_sem, o_sem, sent_x, sent_p, sent_o,
                 xp_r, xb_r, xf_r, st_r, ps_r, sx_r):
    tp = lax.axis_index('tp')
    c = lax.div(tp, 2)
    k = lax.rem(tp, 2)
    oc = 1 - c
    ok = 1 - k
    sib = 2 * c + ok
    par = 2 * oc + k

    def remote(src, dst, ssem, rsem, target):
        return pltpu.make_async_remote_copy(src_ref=src, dst_ref=dst, send_sem=ssem, recv_sem=rsem,
                                            device_id={'tp': target}, device_id_type=MESH)

    def x_load(j):
        return pltpu.make_async_copy(x_h.at[0, :, pl.ds(j * CW, CW)], xa.at[j, c, k], x_sem.at[min(j, 1)])

    for j in range(NC):
        x_load(j).start()
    small = [(g1_h, g1), (g2_h, g2), (bq_h, bq), (bk_h, bk), (bv_h, bv), (pos_h, pos), (freq_h, freq)]
    small_cp = [pltpu.make_async_copy(s, d, sm_sem) for i, (s, d) in enumerate(small)]
    for cp in small_cp:
        cp.start()

    def g_loads(i):
        slot = lax.rem(i, GH)
        rows = pl.ds(pl.multiple_of(i * HW, HW), HW)
        return (pltpu.make_async_copy(wg_h.at[rows], gbuf.at[slot], g_sem.at[slot]),
                pltpu.make_async_copy(wu_h.at[rows], ubuf.at[slot], g_sem.at[slot]))

    def attention_half(wb, wob, qkv):
        def w_loads(j):
            rows = pl.ds(j * CW, CW)
            return (pltpu.make_async_copy(wq_h.at[rows], wb.at[j, :, pl.ds(0, QW)], w_sem.at[j]),
                    pltpu.make_async_copy(wk_h.at[rows], wb.at[j, :, pl.ds(QW, HEAD_DIM)], w_sem.at[j]),
                    pltpu.make_async_copy(wv_h.at[rows], wb.at[j, :, pl.ds(QW + HEAD_DIM, HEAD_DIM)], w_sem.at[j]))

        for j in range(NC):
            for cp in w_loads(j):
                cp.start()
        wo_cp = pltpu.make_async_copy(wo_h, wob, wo_sem)
        wo_cp.start()
        for i in range(GH):
            for cp in g_loads(i):
                cp.start()

        barrier = pltpu.get_barrier_semaphore()
        for peer in (sib, par):
            pl.semaphore_signal(barrier, inc=1, device_id={'tp': peer}, device_id_type=MESH)
        pl.semaphore_wait(barrier, 2)

        def x_to_par(j):
            return remote(xa.at[j, c, k], xa.at[j, c, k], sent_x, xp_r.at[j], par)

        def x_from_par(j):
            return remote(xa.at[j, oc, k], xa.at[j, oc, k], sent_x, xp_r.at[j], par)

        def x_to_sib(j):
            return remote(xa.at[j, c, k], xa.at[j, c, k], sent_x, xb_r.at[j], sib)

        def x_from_sib(j):
            return remote(xa.at[j, c, ok], xa.at[j, c, ok], sent_x, xb_r.at[j], sib)

        def x_forward(j):
            return remote(xa.at[j, oc, k], xa.at[j, oc, k], sent_x, xf_r.at[j], sib)

        def x_forwarded(j):
            return remote(xa.at[j, oc, ok], xa.at[j, oc, ok], sent_x, xf_r.at[j], sib)

        x_load(0).wait()
        x_to_par(0).start()
        x_to_sib(0).start()
        for j in range(1, NC):
            x_load(j).wait()
        square = jnp.zeros((BT, CW), F32)
        for j in range(NC):
            part = xa[j, c, k].astype(F32)
            square = square + part * part
        mean = jnp.sum(square, axis=-1, keepdims=True) / D
        inv = jnp.broadcast_to(lax.rsqrt(mean + NORM_EPS), (BT, 128))
        sta[c, k] = jnp.transpose(jnp.concatenate([inv, inv], axis=0))[:8]
        st_par = remote(sta.at[c, k], sta.at[c, k], sent_x, st_r.at[0], par)
        st_par.start()
        st_sib = remote(sta.at[c, k], sta.at[c, k], sent_x, st_r.at[1], sib)
        st_sib.start()
        for j in range(1, NC):
            x_to_par(j).start()
            x_to_sib(j).start()

        for cp in small_cp:
            cp.wait()
        pos_col = jnp.transpose(jnp.broadcast_to(pos[...].astype(F32), (HEAD_DIM, T)))
        angles = pos_col * freq[...]
        cosine = jnp.cos(angles)
        sine = jnp.sin(angles)
        lane = lax.broadcasted_iota(jnp.int32, (T, HEAD_DIM), 1)
        sine = jnp.where(lane < HEAD_DIM // 2, -sine, sine)

        remote(sta.at[oc, k], sta.at[oc, k], sent_x, st_r.at[0], par).wait_recv()
        st_fwd = remote(sta.at[oc, k], sta.at[oc, k], sent_x, st_r.at[2], sib)
        st_fwd.start()
        remote(sta.at[c, ok], sta.at[c, ok], sent_x, st_r.at[1], sib).wait_recv()
        remote(sta.at[oc, ok], sta.at[oc, ok], sent_x, st_r.at[2], sib).wait_recv()
        for cc in range(2):
            for kk in range(2):
                wide = jnp.broadcast_to(sta[cc, kk][0:1], (128, 128))
                cprev[pl.ds((cc * 2 + kk) * BT, BT), :] = jnp.transpose(wide)[:BT]
        qkv[...] = jnp.zeros_like(qkv)

        def project(j):
            x_from_sib(j).wait_recv()
            x_forwarded(j).wait_recv()
            for cp in w_loads(j):
                cp.wait()
            values = xa[j].reshape(T, CW).astype(F32)
            scale = jnp.concatenate([cprev[...]] * (CW // 128), axis=1)
            gain = row(g1, j * CW, CW)
            hbuf[...] = (values * scale * gain).astype(BF16)
            qkv[...] += dot(hbuf[...], wb[j])

        x_from_par(0).wait_recv()
        x_forward(0).start()

        @pl.loop(1, NC)
        def _(j):
            x_from_par(j).wait_recv()
            x_forward(j).start()
            project(j - 1)

        project(NC - 1)

        def rotate(u, r):
            rows = slice(r * 2 * BT, (r + 1) * 2 * BT)
            return u * cosine[rows] + pltpu.roll(u, HEAD_DIM // 2, 1) * sine[rows]

        half = T // 2
        rows = 4 * half
        row_i = lax.rem(lax.broadcasted_iota(jnp.int32, (rows, half), 0), half)
        causal = row_i >= lax.broadcasted_iota(jnp.int32, (rows, half), 1)
        key_lanes, value_lanes = pl.ds(0, HEAD_DIM), pl.ds(HEAD_DIM, HEAD_DIM)
        for r in range(2):
            width = half * (r + 1)
            part = pl.ds(r * half, half)
            hbuf[part, key_lanes] = rotate(qkv[part, pl.ds(QW, HEAD_DIM)] + row(bk, 0, HEAD_DIM), r).astype(BF16)
            hbuf[part, value_lanes] = (qkv[part, pl.ds(QW + HEAD_DIM, HEAD_DIM)] + row(bv, 0, HEAD_DIM)).astype(BF16)
            for heads in (range(4), range(4, HEADS)):
                stacked = jnp.concatenate([
                    rotate(qkv[part, pl.ds(h * HEAD_DIM, HEAD_DIM)] + row(bq, h * HEAD_DIM, HEAD_DIM), r).astype(BF16)
                    for h in heads], axis=0)
                scores = lax.dot_general(stacked, hbuf[pl.ds(0, width), key_lanes], (((1,), (1,)), ((), ())),
                                         preferred_element_type=F32) * (HEAD_DIM ** -0.5)
                last = jnp.where(causal[:len(heads) * half], scores[:, width - half:], -1e30)
                scores = last if r == 0 else jnp.concatenate([scores[:, :half], last], axis=1)
                weights = jnp.exp(scores - jnp.max(scores, axis=-1, keepdims=True))
                probs = (weights * (1.0 / jnp.sum(weights, axis=-1, keepdims=True))).astype(BF16)
                out = dot(probs, hbuf[pl.ds(0, width), value_lanes]).astype(BF16)
                for i, h in enumerate(heads):
                    obuf[part, pl.ds(h * HEAD_DIM, HEAD_DIM)] = out[i * half:(i + 1) * half]
            if r == 0:
                wo_cp.wait()
            pbuf[0, r] = dot(obuf[part, :], wob[:, pl.ds(0, CW)]).astype(BF16).reshape(2, BT, CW)
            p_sends(0)[r].start()

        k_out = pltpu.make_async_copy(hbuf.at[:, key_lanes], kc_h, o_sem)
        v_out = pltpu.make_async_copy(hbuf.at[:, value_lanes], vc_h, o_sem)
        k_out.start()
        v_out.start()
        chip_partial(0, 0)
        lag = 3
        for j in range(1, NC):
            pbuf[j] = dot(obuf[...], wob[:, pl.ds(j * CW, CW)]).astype(BF16).reshape(2, 2, BT, CW)
            p_sends(j)[0].start()
            if j >= lag:
                chip_partial(j - lag, 1 if j == lag else 0)
        for j in range(NC - lag, NC):
            chip_partial(j, 0)

        @pl.loop(0, NC)
        def _(j):
            x_to_par(j).wait_send()
            x_to_sib(j).wait_send()
            x_forward(j).wait_send()

        st_par.wait_send()
        st_sib.wait_send()
        st_fwd.wait_send()
        k_out.wait()
        v_out.wait()

    def parts(j):
        if isinstance(j, int) and j == 0:
            return ((pl.ds(0, 1), 0), (pl.ds(1, 1), NC))
        return ((pl.ds(0, 2), j),)

    def p_sends(j):
        return [remote(pbuf.at[j, p, ok], psib.at[j, p], sent_p, ps_r.at[i], sib) for p, i in parts(j)]

    def s_sends(j):
        return [remote(sbuf.at[j, p], xs.at[j, p], sent_p, sx_r.at[i], par) for p, i in parts(j)]

    def chip_partial(j, which):
        p = parts(j)[which][0]
        p_sends(j)[which].wait_recv()
        sbuf[j, p] = (pbuf[j, p, k].astype(F32) + psib[j, p].astype(F32)).astype(BF16)
        s_sends(j)[which].start()

    pl.run_scoped(attention_half,
                  pltpu.VMEM((NC, CW, QKV), BF16), pltpu.VMEM((QW, D), BF16), pltpu.VMEM((T, QKV), F32))

    def mlp_half(accg, accu, act, dbuf):
        def d_load(j, slot):
            cols = pl.ds(pl.multiple_of(j * CW, CW), CW)
            return pltpu.make_async_copy(wd_h.at[:, cols], dbuf.at[slot], d_sem.at[slot])

        for s in range(DS):
            d_load(s, s).start()

        def x1_send(j):
            return remote(xa.at[j, :, k], xa.at[j, :, k], sent_o, xb_r.at[j], sib)

        def x1_recv(j):
            return remote(xa.at[j, :, ok], xa.at[j, :, ok], sent_o, xb_r.at[j], sib)

        def residual(j):
            for cp in s_sends(j):
                cp.wait_recv()
            total = sbuf[j].astype(F32) + xs[j].astype(F32)
            xa[j, :, k] = (xa[j, :, k].astype(F32) + total).astype(BF16)
            x1_send(j).start()

        def normalise(u):
            values = xa[u].reshape(T, CW).astype(F32)
            row_sum = jnp.sum(values * values, axis=-1, keepdims=True)
            first = isinstance(u, int) and u == 0
            if not first:
                row_sum = row_sum + ssum[...]
            ssum[...] = row_sum
            scale = lax.rsqrt(row_sum / ((u + 1) * CW) + NORM_EPS)
            wide = jnp.broadcast_to(scale, (T, 128))
            if not first:
                alpha[...] = wide / cprev[...]
            cprev[...] = wide
            hbuf[...] = (values * scale * row(g2, u * CW, CW)).astype(BF16)

        def put(mode, rows, cols, dg, du):
            w = dg.shape[1]
            if mode != 'first':
                al = jnp.concatenate([alpha[rows, :]] * (w // 128), axis=1)
                dg = accg[rows, cols] * al + dg
                du = accu[rows, cols] * al + du
            if mode == 'last':
                act[rows, cols] = (dg / (1.0 + jnp.exp(-dg)) * du).astype(BF16)
            else:
                accg[rows, cols] = dg
                accu[rows, cols] = du

        def tiles(halves, mode, lo, hi):
            for n in range(lo, hi):
                cols = pl.ds(n * TW, TW)
                dg, du = [add([dot(hbuf[:, pl.ds(i * HW, HW)], ref[slot, :, cols]) for i, slot in enumerate(halves)])
                          for ref in (gbuf, ubuf)]
                put(mode, pl.ds(0, T), cols, dg, du)

        def tail(halves, mode):
            cols = pl.ds(FF - 128, 128)
            weight = [jnp.concatenate([gbuf[slot, :, cols], ubuf[slot, :, cols]], axis=1) for slot in halves]
            for r in range(2):
                rows = pl.ds(r * 2 * BT, 2 * BT)
                res = add([dot(hbuf[rows, pl.ds(i * HW, HW)], w) for i, w in enumerate(weight)])
                put(mode, rows, cols, res[:, :128], res[:, 128:])

        NT = FF // TW

        def gate_up(u, mode, cut):
            x1_recv(u).wait_recv()
            for i in range(2):
                for cp in g_loads(2 * u + i):
                    cp.wait()
            halves = [lax.rem(2 * u + i, GH) for i in range(2)]
            if cut == 0:
                residual(u + 1)
            normalise(u)
            if mode == 'last':
                tiles(halves, mode, 0, NT)
            else:
                tiles(halves, mode, 0, cut)
                if cut:
                    residual(u + 1)
                tiles(halves, mode, cut, NT)
            tail(halves, mode)

        def refill(i):
            for cp in g_loads(i):
                cp.start()

        residual(0)
        gate_up(0, 'first', 13)
        for i in range(2):
            refill(GH + i)

        def middle(u, cut):
            gate_up(u, 'mid', cut)
            for i in range(2):
                @pl.when(2 * u + i + GH < 2 * NC)
                def _():
                    refill(2 * u + i + GH)

        pl.loop(1, LATE)(lambda u: middle(u, 9))
        pl.loop(LATE, NC - 1)(lambda u: middle(u, 0))
        gate_up(NC - 1, 'last', NT)

        for j in range(NC):
            for cp in p_sends(j) + s_sends(j):
                cp.wait_send()

        def p2_send(j):
            return remote(pbuf.at[j, :, ok], psib.at[j], sent_o, ps_r.at[j], sib)

        def p2_block(j, block, sem):
            return remote(pbuf.at[j, block, ok], psib.at[j, block], sent_o, ps_r.at[sem], sib)

        def s2_send(j):
            return remote(sbuf.at[j, oc], xs2.at[j], sent_o, xp_r.at[j], par)

        def out_copy(j):
            return pltpu.make_async_copy(sbuf.at[j, c], out_h.at[0, :, pl.ds(pl.multiple_of(j * CW, CW), CW)], o_sem)

        def down(j):
            slot = lax.rem(j, DS)
            d_load(j, slot).wait()
            pbuf[j] = dot(act[...], dbuf[slot]).astype(BF16).reshape(2, 2, BT, CW)
            p2_send(j).start()

        def down_rows(j, block, sem):
            rows = pl.ds(pl.multiple_of(block * 2 * BT, 2 * BT), 2 * BT)
            pbuf[j, block] = dot(act[rows, :], dbuf[j % DS]).astype(BF16).reshape(2, BT, CW)
            p2_block(j, block, sem).start()

        def chip_sum(j, recv):
            recv.wait_recv()
            sbuf[j, oc] = (pbuf[j, oc, k].astype(F32) + psib[j, oc].astype(F32)).astype(BF16)
            s2_send(j).start()

        def finish(j):
            s2_send(j).wait_recv()
            total = pbuf[j, c, k].astype(F32) + psib[j, c].astype(F32) + xs2[j].astype(F32)
            sbuf[j, c] = (xa[j, c, k].astype(F32) + total).astype(BF16)
            out_copy(j).start()

        down(0)
        d_load(DS, 0).start()

        @pl.loop(1, SPLIT)
        def _(j):
            down(j)

            @pl.when(j + DS < NC)
            def _():
                d_load(j + DS, lax.rem(j, DS)).start()

            chip_sum(j - 1, p2_send(j - 1))

        one, two = SPLIT, SPLIT + 1
        d_load(one, one % DS).wait()
        down_rows(one, oc, one)
        chip_sum(one - 1, p2_send(one - 1))
        d_load(two, two % DS).wait()
        down_rows(two, oc, two)
        chip_sum(one, p2_block(one, oc, one))
        down_rows(one, c, NC)
        chip_sum(two, p2_block(two, oc, two))
        down_rows(two, c, NC + 1)
        pl.loop(0, SPLIT)(finish)
        p2_block(one, c, NC).wait_recv()
        finish(one)
        p2_block(two, c, NC + 1).wait_recv()
        finish(two)

        for j in range(NC):
            x1_send(j).wait_send()
            p2_send(j).wait_send()
            s2_send(j).wait_send()
            out_copy(j).wait()

    pl.run_scoped(mlp_half,
                  pltpu.VMEM((T, FF), F32), pltpu.VMEM((T, FF), F32), pltpu.VMEM((T, FF), BF16),
                  pltpu.VMEM((DS, FF, CW), BF16))


def solution(mesh):
    def local_layer(hidden, positions, gain_attn, w_q, b_q, w_k, b_k, w_v, b_v, w_o, gain_mlp, w_gate, w_up, w_down):
        half = HEAD_DIM // 2
        freq = ROPE_THETA ** (-np.arange(half) / half)
        freq = np.concatenate([freq, freq]).reshape(1, HEAD_DIM).astype(np.float32)
        dma = pltpu.SemaphoreType.DMA
        sems = [dma, dma((2,)), dma((NC,)), dma, dma((GH,)), dma((DS,)), dma, dma, dma, dma,
                dma((NO,)), dma((NC,)), dma((NC,)), dma((3,)), dma((NO,)), dma((NC + 1,))]
        vm = pltpu.VMEM
        out, kc, vc = pl.pallas_call(
            layer_kernel,
            out_shape=(jax.ShapeDtypeStruct((1, BT, D), BF16), jax.ShapeDtypeStruct((T, HEAD_DIM), BF16),
                       jax.ShapeDtypeStruct((T, HEAD_DIM), BF16)),
            in_specs=[pl.BlockSpec(memory_space=pl.ANY)] * 15,
            out_specs=(pl.BlockSpec(memory_space=pl.ANY),) * 3,
            scratch_shapes=[
                vm((NC, 2, 2, BT, CW), BF16), vm((2, 2, 8, 128), F32),
                vm((GH, HW, FF), BF16), vm((GH, HW, FF), BF16),
                vm((NC, 2, 2, BT, CW), BF16), vm((NC, 2, BT, CW), BF16), vm((NC, 2, BT, CW), BF16), vm((NC, 2, BT, CW), BF16),
                vm((T, QW), BF16), vm((T, CW), BF16), vm((T, 128), F32), vm((T, 1), F32),
                vm((T, 128), F32), vm((NC, BT, CW), BF16),
                vm((D,), BF16), vm((D,), BF16), vm((QW,), BF16), vm((HEAD_DIM,), BF16), vm((HEAD_DIM,), BF16),
                vm((1, T), jnp.int32), vm((1, HEAD_DIM), F32),
            ] + sems,
            compiler_params=pltpu.CompilerParams(
                collective_id=0, has_side_effects=True, vmem_limit_bytes=67043328),
            name='layer',
        )(hidden, positions, gain_attn, w_q, b_q, w_k, b_k, w_v,
          b_v, w_o, gain_mlp, w_gate, w_up, w_down, freq)
        shapes = (jax.ShapeDtypeStruct((1, BT, D), BF16), jax.ShapeDtypeStruct((T, HEAD_DIM), BF16), jax.ShapeDtypeStruct((T, HEAD_DIM), BF16))
        out, kc, vc = pl.pallas_call(
            result_kernel,
            out_shape=shapes,
            in_specs=[pl.BlockSpec(memory_space=pl.ANY)] * 3,
            out_specs=(pl.BlockSpec(memory_space=pl.ANY),) * 3,
            scratch_shapes=[vm((1, BT, D), BF16), vm((T, HEAD_DIM), BF16), vm((T, HEAD_DIM), BF16), dma, dma],
            name='results',
        )(out, kc, vc)
        return out, kc.reshape(1, T, 1, HEAD_DIM), vc.reshape(1, T, 1, HEAD_DIM)

    token_rows = P('dp', 'tp', None)
    col_split = P(None, 'tp')
    row_split = P('tp', None)
    vec_split = P('tp')
    replicated = P(None)
    cache_spec = P('dp', None, 'tp', None)
    in_specs = (token_rows, P('dp', None), replicated, col_split, vec_split, col_split, vec_split, col_split, vec_split, row_split, replicated, col_split, col_split, row_split)
    out_specs = (token_rows, cache_spec, cache_spec)
    return jax.shard_map(local_layer, mesh=mesh, in_specs=in_specs, out_specs=out_specs, check_vma=False)
```
